256 devices in a mesh: cells: 32 (over z, x), genes: 8 (over y, core).
Axes of the slice: x: 4, y: 4, z: 8, core: 2. Of those that a mesh axis runs over, the one named last changes fastest.
Arguments:
- counts: int32 [155648, 4000], P('cells', 'genes'), may hold values from 0 to 674, as said below
- sketch: bfloat16 [4000, 128], P('genes'), may hold values from -6 to 6
Outputs:
- basis: float32 [155648, 128], P('cells')
- loadings: float32 [4000, 128], P('genes')
The draws below stay inside these ranges and needn't reach their ends.
Inputs may be any that keep to these rules, and one draw needn't show every extreme that they name: `counts`: every cell and every gene has a positive total.
All inputs are finite; a program needn't handle non-finite values.
Results may differ from the reference program's by a relative error of at most 0.0051.
Values may be sent and summed in bfloat16 or wider, within the bound.
A program may use at most 128 MiB of HBM per device.

```python
import math
import jax
import jax.numpy as jnp
from jax import lax

CELL_DEV = 4864
GENES = 4000
RANK = 128
ITERS = 2
CELLS = 155648
N_CELLS = 32


def draw_counts(key, part):
    subkeys = jax.random.split(key, 4)
    row_ids = jnp.arange(CELLS, dtype=jnp.int32)[:, None]
    col_ids = jnp.arange(GENES, dtype=jnp.int32)[None, :]
    level_exp = jax.random.randint(subkeys[0], (1, GENES), 0, 2)
    gene_level = jnp.left_shift(jnp.int32(1), level_exp) * (12 * col_ids // GENES + 1)
    cell_level = jax.random.randint(subkeys[1], (CELLS, 1), 1, 4) * (6 * row_ids // CELLS + 2)
    ceiling = (gene_level * cell_level + 15) // 16
    background = jax.random.randint(subkeys[2], (CELLS, GENES), 0, ceiling + 1)
    marker = (col_ids == row_ids % GENES).astype(jnp.int32)
    rolled = jax.random.randint(subkeys[3], (CELLS, GENES), 0, 6400 * GENES)
    spikes = jnp.where(rolled < 400, 200 + rolled, 0)
    return (background + marker + spikes).astype(jnp.int32)


def block_scale(rng, extent, pieces, low, high):
    loudness = 1.0
    for position, shards_of in pieces:
        steps = jax.random.uniform(jax.random.fold_in(jax.random.fold_in(rng, 6), position), (shards_of,), jnp.float32, low / len(pieces), high / len(pieces))
        loudness = loudness * jnp.repeat(jnp.exp(steps), extent[position] // shards_of).reshape((-1,) + (1,) * (len(extent) - 1 - position))
    return loudness


def centred(key, extent, scale, most, cuts=(), kind=jnp.bfloat16):
    values = scale * jax.random.normal(key, extent, jnp.float32)
    if cuts:
        values = values * block_scale(key, extent, cuts, -0.22, 0.18)
    return jnp.clip(values, -most, most).astype(kind)


def setup_inputs(seed: int = 0) -> dict:
    key_list = jax.random.split(jax.random.key(seed), 3)
    return {
        "counts": draw_counts(jax.random.fold_in(key_list[2], 71), 0),
        "sketch": centred(key_list[1], (GENES, RANK), 1.0, 6.0, ((0, 8),)),
    }


def residual_block(block, cell_total, frac, limit):
    values = block.astype(jnp.float32)
    expected = cell_total[:, None] * frac[None, :]
    scaled = (values - expected) / jnp.sqrt(expected + 0.01 * expected * expected)
    return jnp.clip(scaled, -limit, limit).astype(jnp.bfloat16)

def self_gram(block):
    return lax.dot_general(block.astype(jnp.float32), block.astype(jnp.float32), (((0,), (0,)), ((), ())), precision=lax.Precision.HIGHEST, preferred_element_type=jnp.float32)

def whitening(gram, count):
    width = gram.shape[0]
    identity = jnp.eye(width, dtype=jnp.float32)
    shifted = gram + 1e-05 * jnp.trace(gram) / width * identity
    lower = jnp.linalg.cholesky(shifted)
    inverse = jax.scipy.linalg.solve_triangular(lower, identity, lower=True)
    return jnp.transpose(inverse) * math.sqrt(count)

def reference(counts, sketch):
    cell_total = lax.optimization_barrier(jnp.sum(counts, axis=1)).astype(jnp.float32)
    gene_total = lax.optimization_barrier(jnp.sum(counts, axis=0)).astype(jnp.float32)
    grand = jnp.sum(gene_total)
    frac = gene_total / grand
    limit = math.sqrt(float(CELLS))
    blocks = counts.reshape(N_CELLS, CELL_DEV, GENES)
    cell_blocks = cell_total.reshape(N_CELLS, CELL_DEV)
    gene_scale = math.sqrt(float(GENES)) / float(CELLS)
    omega = sketch
    basis = None
    loadings = None
    for sweep in range(ITERS):

        def sketch_block(operands, omega=omega):
            resid = residual_block(operands[0], operands[1], frac, limit)
            return jnp.dot(resid.astype(jnp.float32), omega.astype(jnp.float32), preferred_element_type=jnp.float32)
        sketched = lax.map(sketch_block, (blocks, cell_blocks)).reshape(CELLS, RANK)
        basis = jnp.dot(sketched, whitening(self_gram(sketched), float(CELLS)), precision=lax.Precision.HIGHEST)
        basis_blocks = basis.astype(jnp.bfloat16).reshape(N_CELLS, CELL_DEV, RANK)

        def add_block(total, operands):
            resid = residual_block(operands[0], operands[1], frac, limit)
            term = lax.dot_general(resid.astype(jnp.float32), operands[2].astype(jnp.float32), (((0,), (0,)), ((), ())), preferred_element_type=jnp.float32)
            return (total + term, None)
        start_total = jnp.zeros((GENES, RANK), jnp.float32)
        summed, _ = lax.scan(add_block, start_total, (blocks, cell_blocks, basis_blocks))
        loadings = summed * gene_scale
        if sweep < ITERS - 1:
            omega = loadings.astype(jnp.bfloat16)
    return (basis, loadings)
```

```python
import functools
import math

import jax
import jax.numpy as jnp
from jax import lax
from jax.experimental import pallas as pl
from jax.experimental.pallas import tpu as pltpu
from jax.sharding import PartitionSpec as P

ITERS = 2
NX = 4
NK = 2
TILE = 128
STEP = 32
PANEL = 8
HIGHEST = lax.Precision.HIGHEST
MESH = pl.DeviceIdType.MESH
F32 = jnp.float32
BF16 = jnp.bfloat16


def outer_contract(left, right, precision=None):
    return lax.dot_general(
        left, right, (((0,), (0,)), ((), ())), precision=precision, preferred_element_type=F32
    )


def kernel(
    dims,
    counts_hbm,
    sketch_ref,
    s_out,
    w_out,
    load_out,
    cnt,
    res,
    ct,
    cellx,
    totc,
    genex,
    genez,
    grp,
    fracs,
    omega,
    psend,
    precv,
    pown,
    qbuf,
    fbuf,
    rbuf,
    sfull,
    tacc,
    gacc,
    txs,
    txr,
    tzs,
    tzr,
    tall,
    gx,
    gz,
    gg,
    aug,
    linv,
    load_sem,
    out_sem,
    bx_ss,
    bx_rs,
    bz_ss,
    bz_rs,
    ba_ss,
    ba_rs,
    bg_ss,
    bg_rs,
    pr_ss,
    pr_rs,
    f_ss,
    f_rs,
    r_ss,
    r_rs,
    ag_ss,
    ag_rs,
    tx_ss,
    tx_rs,
    tz_ss,
    tz_rs,
    taz_ss,
    taz_rs,
    tax_ss,
    tax_rs,
    gx_ss,
    gx_rs,
    gz_ss,
    gz_rs,
    gg_ss,
    gg_rs,
):
    nx, nz, ng, rows, genes, wide, rank, n_cells, n_genes = dims
    ny = ng // NK
    shard = rows // ng
    half = shard // 2
    tiles = rows // TILE
    blk = wide // nx
    zr = rank // nz
    gr = rank // ng
    me_c = lax.axis_index("cells")
    me_g = lax.axis_index("genes")
    mz, mx = me_c // nx, lax.rem(me_c, nx)
    my, mk = me_g // NK, lax.rem(me_g, NK)
    ok = 1 - mk
    y_up, y_dn, y_far = (lax.rem(my + d, ny) for d in (1, 3, 2))

    def copy(src, dst, ss, rs, c, g):
        return pltpu.make_async_remote_copy(
            src_ref=src, dst_ref=dst, send_sem=ss, recv_sem=rs, device_id=(c, g), device_id_type=MESH
        )

    def x_peer(i):
        return mz * nx + i, me_g

    def z_peer(i):
        return i * nx + mx, me_g

    def g_peer(i):
        return me_c, i

    sent = []

    def spread(n, me, peer, src_of, dst, ss, rs):
        arrivals = []
        for d in range(1, n):
            to, frm = lax.rem(me + d, n), lax.rem(me + n - d, n)
            out = copy(src_of(to), dst.at[me], ss.at[d], rs.at[d], *peer(to))
            out.start()
            sent.append(out)
            arrivals.append(copy(src_of(to), dst.at[frm], ss.at[d], rs.at[d], *peer(to)))
        return arrivals

    def wait_all(arrivals):
        for a in arrivals:
            a.wait_recv()

    def total(slots, n):
        acc = slots[0]
        for i in range(1, n):
            acc = acc + slots[i]
        return acc

    barrier = pltpu.get_barrier_semaphore()
    for n, me, peer in ((nx, mx, x_peer), (nz, mz, z_peer), (ng, me_g, g_peer)):
        for d in range(1, n):
            pl.semaphore_signal(barrier, inc=1, device_id=peer(lax.rem(me + d, n)), device_id_type=MESH)

    per = 2 * TILE if tiles % 2 == 0 else TILE
    loads = []
    for i in range(rows // per):
        part = pl.ds(i * per, per)
        loads.append(pltpu.make_async_copy(counts_hbm.at[part], cnt.at[part], load_sem.at[i]))
        loads[-1].start()

    omega[pl.ds(wide - TILE, TILE), :] = jnp.zeros((TILE, rank), BF16)
    omega[pl.ds(0, genes), :] = sketch_ref[...]

    groups = wide // TILE
    spare = wide - genes

    def lanes(r, n):
        out = []
        for g in range(groups):
            if g < groups - 1:
                out.append(cnt[pl.ds(r, n), pl.ds(g * TILE, TILE)].astype(F32))
            else:
                last = cnt[pl.ds(r, n), pl.ds(g * TILE, TILE - spare)].astype(F32)
                out.append(jnp.concatenate([last, jnp.zeros((n, spare), F32)], axis=1))
        return out

    cols = tuple(jnp.zeros((8, TILE), F32) for _ in range(groups))
    sub = per // TILE

    def stats(i, cols):
        part = pl.ds(pl.multiple_of(i * per, per), per)
        pltpu.make_async_copy(counts_hbm.at[part], cnt.at[part], load_sem.at[i]).wait()
        for j in range(sub):
            xs = lanes(pl.multiple_of(i * per + j * TILE, TILE), TILE)
            cols = tuple(c + jnp.sum(x.reshape(TILE // 8, 8, TILE), axis=0) for c, x in zip(cols, xs))
            line = xs[0]
            for x in xs[1:]:
                line = line + x
            across = jnp.sum(jnp.transpose(line), axis=0, keepdims=True)
            cellx[me_g, pl.ds(i * sub + j, 1), :] = across
        return cols

    cols = lax.fori_loop(0, rows // per, stats, cols)
    for g in range(groups):
        genex[mx, :, pl.ds(g * TILE, TILE)] = jnp.sum(cols[g], axis=0, keepdims=True)

    pl.semaphore_wait(barrier, nx + nz + ng - 3)
    got_x = spread(nx, mx, x_peer, lambda to: genex.at[mx], genex, bx_ss, bx_rs)
    got_a = spread(ng, me_g, g_peer, lambda to: cellx.at[me_g], cellx, ba_ss, ba_rs)
    wait_all(got_x)
    genez[mz] = total(genex, nx)
    got_z = spread(nz, mz, z_peer, lambda to: genez.at[mz], genez, bz_ss, bz_rs)
    wait_all(got_a)
    totc[...] = total(cellx, ng)

    def widen(t, carry):
        line = jnp.broadcast_to(totc[pl.ds(t, 1), :], (TILE, TILE))
        ct[pl.ds(pl.multiple_of(t * TILE, TILE), TILE), :] = jnp.transpose(line)
        return carry

    lax.fori_loop(0, tiles, widen, 0)
    wait_all(got_z)
    gene_total = total(genez, nz)
    short = gene_total[:, :TILE]
    for g in range(1, groups):
        short = short + gene_total[:, g * TILE : (g + 1) * TILE]
    grp[me_g] = short
    wait_all(spread(ng, me_g, g_peer, lambda to: grp.at[me_g], grp, bg_ss, bg_rs))
    grand = jnp.sum(total(grp, ng), axis=1, keepdims=True)
    fill = lax.broadcasted_iota(jnp.int32, (1, wide), 1) >= genes
    fracs[...] = jnp.where(fill, 1.0, gene_total / grand)

    limit = math.sqrt(n_cells)

    def residuals(base):
        def some(i, carry):
            r = pl.multiple_of(base + i * STEP, STEP)
            cell = ct[pl.ds(r, STEP), :]
            xs = lanes(r, STEP)
            for g in range(groups):
                mu = cell * fracs[:, pl.ds(g * TILE, TILE)]
                value = (xs[g] - mu) * lax.rsqrt(mu + 0.01 * mu * mu)
                value = jnp.clip(value, -limit, limit)
                if g == groups - 1:
                    lane = lax.broadcasted_iota(jnp.int32, (STEP, TILE), 1)
                    value = jnp.where(lane < TILE - spare, value, 0.0)
                res[pl.ds(r, STEP), pl.ds(g * TILE, TILE)] = value.astype(BF16)
            return carry

        lax.fori_loop(0, shard // STEP, some, 0)

    gene_scale = math.sqrt(n_genes) / n_cells

    def whiten(it):
        eye = (
            lax.broadcasted_iota(jnp.int32, (rank, rank), 0)
            == lax.broadcasted_iota(jnp.int32, (rank, rank), 1)
        )
        gram = jnp.concatenate([gg[it, i] for i in range(ng)], axis=0)
        diagonal = jnp.sum(jnp.sum(jnp.where(eye, gram, 0.0), axis=1, keepdims=True), axis=0, keepdims=True)
        aug[:, pl.ds(0, rank)] = gram + jnp.where(eye, 1e-05 * diagonal / rank, 0.0)
        aug[:, pl.ds(rank, rank)] = jnp.where(eye, 1.0, 0.0)
        lane = lax.broadcasted_iota(jnp.int32, (PANEL, rank), 1)
        row = lax.broadcasted_iota(jnp.int32, (PANEL, 2 * rank), 0)

        def panel(p, carry):
            j = pl.multiple_of(p * PANEL, PANEL)
            lines = aug[pl.ds(j, PANEL), :]
            left = lines[:, :rank]
            heads = [
                jnp.sum(jnp.where(lane == j + i, left, 0.0), axis=1, keepdims=True) for i in range(PANEL)
            ]
            for i in range(PANEL):
                inv = lax.rsqrt(heads[i][i : i + 1, :])
                col = heads[i] * inv
                for m in range(i + 1, PANEL):
                    heads[m] = heads[m] - col * col[m : m + 1, :]
                this = lines[i : i + 1, :] * inv
                lines = jnp.where(row > i, lines - col * this, jnp.where(row == i, this, lines))
            linv[pl.ds(j, PANEL), :] = lines[:, rank:]
            aug[...] = aug[...] - outer_contract(lines[:, :rank], lines, HIGHEST)
            return carry

        lax.fori_loop(0, rank // PANEL, panel, 0)
        return jnp.transpose(linv[...]) * math.sqrt(n_cells)

    for it in range(ITERS):
        order = (y_far, y_up, y_dn, my)

        def pair(n):
            for k in (ok, mk):
                base = pl.multiple_of((order[n] * NK + k) * shard, 16)
                if it == 0:
                    residuals(base)
                part = jnp.dot(res[pl.ds(base, shard), :], omega[...], preferred_element_type=F32)
                if k is ok:
                    psend[it, n] = part
                    out = copy(
                        psend.at[it, n], precv.at[it, n], pr_ss.at[it, n], pr_rs.at[it, n], *g_peer(my * NK + ok)
                    )
                    out.start()
                    sent.append(out)
                else:
                    pown[n] = part

        def both(n):
            copy(
                psend.at[it, n], precv.at[it, n], pr_ss.at[it, n], pr_rs.at[it, n], *g_peer(my * NK + ok)
            ).wait_recv()
            return pown[n] + precv[it, n]

        up, dn = g_peer(y_up * NK + mk), g_peer(y_dn * NK + mk)
        other = g_peer(my * NK + ok)
        top, bot = pl.ds(0, half), pl.ds(half, half)

        pair(0)
        pair(1)
        qbuf[it, 0] = both(0).astype(BF16)
        far_up = copy(qbuf.at[it, 0, top], fbuf.at[it, 0], f_ss.at[it, 0], f_rs.at[it, 0], *up)
        far_dn = copy(qbuf.at[it, 0, bot], fbuf.at[it, 1], f_ss.at[it, 1], f_rs.at[it, 1], *dn)
        far_up.start()
        far_dn.start()
        pair(2)
        q = both(1)
        far_up.wait_recv()
        qbuf[it, 1, top] = (q[:half] + fbuf[it, 0].astype(F32)).astype(BF16)
        qbuf[it, 1, bot] = q[half:].astype(BF16)
        near_up = copy(qbuf.at[it, 1], rbuf.at[it, 0], r_ss.at[it, 0], r_rs.at[it, 0], *up)
        near_up.start()
        q = both(2)
        far_dn.wait_recv()
        qbuf[it, 2, top] = q[:half].astype(BF16)
        qbuf[it, 2, bot] = (q[half:] + fbuf[it, 1].astype(F32)).astype(BF16)
        near_dn = copy(qbuf.at[it, 2], rbuf.at[it, 1], r_ss.at[it, 1], r_rs.at[it, 1], *dn)
        near_dn.start()
        pair(3)
        own = both(3)
        near_up.wait_recv()
        near_dn.wait_recv()
        sfull[it, me_g] = (own + rbuf[it, 0].astype(F32) + rbuf[it, 1].astype(F32)).astype(BF16)
        sent.extend([far_up, far_dn, near_up, near_dn])

        def block(g, part=None):
            return sfull.at[it, g] if part is None else sfull.at[it, g, part]

        def send(n, g, part, peer):
            out = copy(block(g, part), block(g, part), ag_ss.at[it, n], ag_rs.at[it, n], *peer)
            out.start()
            sent.append(out)

        def arrive(n, g, part):
            copy(block(g, part), block(g, part), ag_ss.at[it, n], ag_rs.at[it, n], *other).wait_recv()

        mine = me_g
        up_k, dn_k, far_k = (y * NK + mk for y in (y_up, y_dn, y_far))
        up_o, dn_o, far_o = (y * NK + ok for y in (y_up, y_dn, y_far))
        mine_o = my * NK + ok

        def gather(first, g):
            base = pl.multiple_of(g * shard, 16)
            s = sfull[it, g]
            t = outer_contract(s, res[pl.ds(base, shard), :])
            u = outer_contract(s, s)
            if first:
                tacc[it] = t
                gacc[it] = u
            else:
                tacc[it] = tacc[it] + t
                gacc[it] = gacc[it] + u

        send(0, mine, top, up)
        send(1, mine, bot, dn)
        send(2, mine, bot, up)
        send(3, mine, top, dn)
        send(4, mine, None, other)
        gather(True, mine)
        arrive(0, dn_k, top)
        send(5, dn_k, top, up)
        arrive(1, up_k, bot)
        send(6, up_k, bot, dn)
        arrive(4, mine_o, None)
        gather(False, mine_o)
        arrive(2, dn_k, bot)
        send(7, dn_k, None, other)
        arrive(3, up_k, top)
        send(8, up_k, None, other)
        gather(False, dn_k)
        gather(False, up_k)
        arrive(7, dn_o, None)
        gather(False, dn_o)
        arrive(8, up_o, None)
        gather(False, up_o)
        arrive(5, far_k, top)
        arrive(6, far_k, bot)
        send(9, far_k, None, other)
        gather(False, far_k)
        arrive(9, far_o, None)
        gather(False, far_o)
        if it == ITERS - 1:
            leave = pltpu.make_async_copy(sfull.at[it], s_out, out_sem)
            leave.start()

        for i in range(nx):
            txs[it, i] = tacc[it, :, pl.ds(i * blk, blk)]
        txr[it, mx] = txs[it, mx]
        gx[it, mx] = gacc[it, pl.ds(pl.multiple_of(me_g * gr, 8), gr), :]
        got_gx = spread(nx, mx, x_peer, lambda to: gx.at[it, mx], gx.at[it], gx_ss.at[it], gx_rs.at[it])
        got_tx = spread(nx, mx, x_peer, lambda to: txs.at[it, to], txr.at[it], tx_ss.at[it], tx_rs.at[it])
        wait_all(got_gx)
        gz[it, mz] = total([gx[it, i] for i in range(nx)], nx)
        got_gz = spread(nz, mz, z_peer, lambda to: gz.at[it, mz], gz.at[it], gz_ss.at[it], gz_rs.at[it])
        wait_all(got_tx)
        tsum = total([txr[it, i] for i in range(nx)], nx)
        for i in range(nz):
            tzs[it, i] = tsum[i * zr : (i + 1) * zr, :]
        tzr[it, mz] = tzs[it, mz]
        got_tz = spread(nz, mz, z_peer, lambda to: tzs.at[it, to], tzr.at[it], tz_ss.at[it], tz_rs.at[it])
        wait_all(got_gz)
        gg[it, me_g] = total([gz[it, i] for i in range(nz)], nz)
        got_gg = spread(ng, me_g, g_peer, lambda to: gg.at[it, me_g], gg.at[it], gg_ss.at[it], gg_rs.at[it])
        wait_all(got_tz)
        tall[it, mx, mz] = total([tzr[it, i] for i in range(nz)], nz)
        got_taz = spread(
            nz, mz, z_peer, lambda to: tall.at[it, mx, mz], tall.at[it, mx], taz_ss.at[it], taz_rs.at[it]
        )
        wait_all(got_gg)
        white = whiten(it)
        wait_all(got_taz)
        got_tax = spread(
            nx, mx, x_peer, lambda to: tall.at[it, mx], tall.at[it], tax_ss.at[it], tax_rs.at[it]
        )
        if it == ITERS - 1:
            w_out[...] = white
        wait_all(got_tax)
        for i in range(nx):
            t = jnp.concatenate([tall[it, i, j] for j in range(nz)], axis=0)
            loading = outer_contract(t, white, HIGHEST) * gene_scale
            if it == ITERS - 1:
                load_out[pl.ds(i * blk, blk), :] = loading
            else:
                omega[pl.ds(i * blk, blk), :] = loading.astype(BF16)

    leave.wait()
    for s in sent:
        s.wait_send()


def shards(counts, sketch):
    rows, genes = counts.shape
    rank = sketch.shape[1]
    nc, ng = lax.axis_size("cells"), lax.axis_size("genes")
    nx = NX
    nz = nc // nx
    wide = -(-genes // TILE) * TILE
    shard = rows // ng
    tiles = rows // TILE
    blk, zr, gr = wide // nx, rank // nz, rank // ng
    dims = (nx, nz, ng, rows, genes, wide, rank, nc * rows, ng * genes)
    per = 2 * TILE if tiles % 2 == 0 else TILE
    V = pltpu.VMEM
    D = pltpu.SemaphoreType.DMA

    def pairs(*shape):
        return [D(shape), D(shape)]

    s_all, white, load = pl.pallas_call(
        functools.partial(kernel, dims),
        out_shape=(
            jax.ShapeDtypeStruct((ng, shard, rank), BF16),
            jax.ShapeDtypeStruct((rank, rank), F32),
            jax.ShapeDtypeStruct((wide, rank), F32),
        ),
        in_specs=[pl.BlockSpec(memory_space=pl.ANY), pl.BlockSpec(memory_space=pltpu.VMEM)],
        out_specs=(
            pl.BlockSpec(memory_space=pl.ANY),
            pl.BlockSpec(memory_space=pltpu.VMEM),
            pl.BlockSpec(memory_space=pltpu.VMEM),
        ),
        scratch_shapes=[
            V((rows, genes), jnp.int32),
            V((rows, wide), BF16),
            V((rows, TILE), F32),
            V((ng, tiles, TILE), F32),
            V((tiles, TILE), F32),
            V((nx, 1, wide), F32),
            V((nz, 1, wide), F32),
            V((ng, 1, TILE), F32),
            V((1, wide), F32),
            V((wide, rank), BF16),
            V((ITERS, 4, shard, rank), F32),
            V((ITERS, 4, shard, rank), F32),
            V((4, shard, rank), F32),
            V((ITERS, 3, shard, rank), BF16),
            V((ITERS, 2, shard // 2, rank), BF16),
            V((ITERS, 2, shard, rank), BF16),
            V((ITERS, ng, shard, rank), BF16),
            V((ITERS, rank, wide), F32),
            V((ITERS, rank, rank), F32),
            V((ITERS, nx, rank, blk), F32),
            V((ITERS, nx, rank, blk), F32),
            V((ITERS, nz, zr, blk), F32),
            V((ITERS, nz, zr, blk), F32),
            V((ITERS, nx, nz, zr, blk), F32),
            V((ITERS, nx, gr, rank), F32),
            V((ITERS, nz, gr, rank), F32),
            V((ITERS, ng, gr, rank), F32),
            V((rank, 2 * rank), F32),
            V((rank, rank), F32),
            D((rows // per,)),
            D,
            *pairs(nx),
            *pairs(nz),
            *pairs(ng),
            *pairs(ng),
            *pairs(ITERS, 4),
            *pairs(ITERS, 2),
            *pairs(ITERS, 2),
            *pairs(ITERS, 10),
            *pairs(ITERS, nx),
            *pairs(ITERS, nz),
            *pairs(ITERS, nz),
            *pairs(ITERS, nx),
            *pairs(ITERS, nx),
            *pairs(ITERS, nz),
            *pairs(ITERS, ng),
        ],
        compiler_params=pltpu.CompilerParams(
            collective_id=0, has_side_effects=True, vmem_limit_bytes=60 * 2**20
        ),
        name="sweep",
    )(counts, sketch)
    basis = jnp.dot(s_all.reshape(rows, rank).astype(F32), white, precision=HIGHEST)
    return basis, load[:genes]


def solution(mesh):
    return jax.shard_map(
        shards,
        mesh=mesh,
        in_specs=(P("cells", "genes"), P("genes", None)),
        out_specs=(P("cells", None), P("genes", None)),
        check_vma=False,
    )
```

```python
import functools
import math

import jax
import jax.numpy as jnp
from jax import lax
from jax.experimental import pallas as pl
from jax.experimental.pallas import tpu as pltpu
from jax.sharding import PartitionSpec as P

ITERS = 2
NX = 4
NK = 2
TILE = 128
STEP = 32
PANEL = 8
PER = 2
HIGHEST = lax.Precision.HIGHEST
MESH = pl.DeviceIdType.MESH
F32 = jnp.float32
BF16 = jnp.bfloat16


def outer_contract(left, right, precision=None):
    return lax.dot_general(
        left, right, (((0,), (0,)), ((), ())), precision=precision, preferred_element_type=F32
    )


def inner_contract(left, right, precision=None):
    return lax.dot_general(
        left, right, (((1,), (1,)), ((), ())), precision=precision, preferred_element_type=F32
    )


def kernel(
    dims,
    counts_hbm,
    sketch_ref,
    s_out,
    w_out,
    load_out,
    cnt,
    res,
    gpart,
    cellx,
    totc,
    genex,
    genez,
    grp,
    fracs,
    omega,
    psend,
    precv,
    pown,
    qbuf,
    fbuf,
    rbuf,
    sfull,
    tacc,
    gacc,
    txs,
    txr,
    tzs,
    tzr,
    tall,
    gx,
    gz,
    gg,
    aug,
    linv,
    load_sem,
    out_sem,
    bx_ss,
    bx_rs,
    bz_ss,
    bz_rs,
    ba_ss,
    ba_rs,
    bg_ss,
    bg_rs,
    pr_ss,
    pr_rs,
    f_ss,
    f_rs,
    r_ss,
    r_rs,
    ag_ss,
    ag_rs,
    tx_ss,
    tx_rs,
    tz_ss,
    tz_rs,
    taz_ss,
    taz_rs,
    tax_ss,
    tax_rs,
    gx_ss,
    gx_rs,
    gz_ss,
    gz_rs,
    gg_ss,
    gg_rs,
):
    nx, nz, ng, rows, genes, wide, rank, n_cells, n_genes = dims
    ny = ng // NK
    shard = shard_of(rows, ng)
    half = rank // 2
    blk = wide // nx
    zr = blk // nz
    gr = rank // ng
    me_c = lax.axis_index("cells")
    me_g = lax.axis_index("genes")
    mz, mx = me_c // nx, lax.rem(me_c, nx)
    my, mk = me_g // NK, lax.rem(me_g, NK)
    ok = 1 - mk
    y_up, y_dn, y_far = (lax.rem(my + d, ny) for d in (1, 3, 2))

    def copy(src, dst, ss, rs, c, g):
        return pltpu.make_async_remote_copy(
            src_ref=src, dst_ref=dst, send_sem=ss, recv_sem=rs, device_id=(c, g), device_id_type=MESH
        )

    def x_peer(i):
        return mz * nx + i, me_g

    def z_peer(i):
        return i * nx + mx, me_g

    def g_peer(i):
        return me_c, i

    sent = []

    def spread(n, me, peer, src_of, dst, ss, rs):
        arrivals = []
        for d in range(1, n):
            to, frm = lax.rem(me + d, n), lax.rem(me + n - d, n)
            out = copy(src_of(to), dst.at[me], ss.at[d], rs.at[d], *peer(to))
            out.start()
            sent.append(out)
            arrivals.append(copy(src_of(to), dst.at[frm], ss.at[d], rs.at[d], *peer(to)))
        return arrivals

    def wait_all(arrivals):
        for a in arrivals:
            a.wait_recv()

    def total(slots, n):
        acc = slots[0]
        for i in range(1, n):
            acc = acc + slots[i]
        return acc

    barrier = pltpu.get_barrier_semaphore()
    for n, me, peer in ((nx, mx, x_peer), (nz, mz, z_peer), (ng, me_g, g_peer)):
        for d in range(1, n):
            pl.semaphore_signal(barrier, inc=1, device_id=peer(lax.rem(me + d, n)), device_id_type=MESH)

    per = PER * TILE
    loads = rows // per

    def load(i):
        part = pl.ds(pl.multiple_of(i * per, TILE), per)
        return pltpu.make_async_copy(counts_hbm.at[:, part], cnt.at[:, part], load_sem.at[i])

    for i in range(loads):
        load(i).start()

    res[:, pl.ds(rows, ng * shard - rows)] = jnp.zeros((wide, ng * shard - rows), BF16)
    flip = jnp.transpose(sketch_ref[...].astype(F32))
    omega[...] = jnp.concatenate([flip, jnp.zeros((rank, wide - genes), F32)], axis=1).astype(BF16)
    gpart[...] = jnp.zeros((genes, TILE), jnp.int32)
    even = genes - genes % 8

    def stats(i, carry):
        load(i).wait()
        tot = None
        for j in range(PER):
            at = pl.multiple_of(i * per + j * TILE, TILE)
            x = cnt[:, pl.ds(at, TILE)]
            tot = x if tot is None else tot + x
            down = jnp.sum(x[:even].reshape(even // 8, 8, TILE), axis=0)
            down = jnp.sum(down, axis=0, keepdims=True)
            if even < genes:
                down = down + jnp.sum(x[even:], axis=0, keepdims=True)
            cellx[me_g, :, pl.ds(at, TILE)] = down.astype(F32)
        gpart[...] = gpart[...] + tot
        return carry

    lax.fori_loop(0, loads, stats, 0)
    groups = wide // TILE
    for g in range(groups):
        n = min(TILE, genes - g * TILE)
        line = gpart[pl.ds(g * TILE, n), :].astype(F32)
        if n < TILE:
            line = jnp.concatenate([line, jnp.zeros((TILE - n, TILE), F32)], axis=0)
        genex[mx, :, pl.ds(g * TILE, TILE)] = jnp.sum(jnp.transpose(line), axis=0, keepdims=True)

    pl.semaphore_wait(barrier, nx + nz + ng - 3)
    got_x = spread(nx, mx, x_peer, lambda to: genex.at[mx], genex, bx_ss, bx_rs)
    got_a = spread(ng, me_g, g_peer, lambda to: cellx.at[me_g], cellx, ba_ss, ba_rs)
    wait_all(got_x)
    genez[mz] = total(genex, nx)
    got_z = spread(nz, mz, z_peer, lambda to: genez.at[mz], genez, bz_ss, bz_rs)
    wait_all(got_a)
    totc[...] = total(cellx, ng)
    wait_all(got_z)
    gene_total = total(genez, nz)
    short = gene_total[:, :TILE]
    for g in range(1, groups):
        short = short + gene_total[:, g * TILE : (g + 1) * TILE]
    grp[me_g] = short
    got_g = spread(ng, me_g, g_peer, lambda to: grp.at[me_g], grp, bg_ss, bg_rs)
    fill = lax.broadcasted_iota(jnp.int32, (1, wide), 1) >= genes
    gene_total = jnp.where(fill, 1.0, gene_total)
    for g in range(groups):
        line = jnp.broadcast_to(gene_total[:, g * TILE : (g + 1) * TILE], (TILE, TILE))
        fracs[pl.ds(g * TILE, TILE), :] = jnp.transpose(line)
    wait_all(got_g)
    grand = jnp.sum(total(grp, ng), axis=1, keepdims=True)
    fracs[...] = fracs[...] / grand

    limit = math.sqrt(n_cells)

    def residuals(g):
        def some(t, carry):
            at = pl.ds(pl.multiple_of(t * TILE, TILE), TILE)
            cell = totc[:, at]
            for k in range(wide // STEP):
                n = min(STEP, genes - k * STEP)
                x = cnt[pl.ds(k * STEP, n), at].astype(F32)
                if n < STEP:
                    x = jnp.concatenate([x, jnp.zeros((STEP - n, TILE), F32)], axis=0)
                mu = cell * fracs[pl.ds(k * STEP, STEP), :]
                value = (x - mu) * lax.rsqrt(mu + 0.01 * mu * mu)
                value = jnp.clip(value, -limit, limit)
                if n < STEP:
                    row = lax.broadcasted_iota(jnp.int32, (STEP, TILE), 0)
                    value = jnp.where(row < n, value, 0.0)
                res[pl.ds(k * STEP, STEP), at] = value.astype(BF16)
            return carry

        first = g * (shard // TILE)
        lax.fori_loop(first, jnp.minimum(first + shard // TILE, rows // TILE), some, 0)

    gene_scale = math.sqrt(n_genes) / n_cells

    def whiten(it):
        eye = (
            lax.broadcasted_iota(jnp.int32, (rank, rank), 0)
            == lax.broadcasted_iota(jnp.int32, (rank, rank), 1)
        )
        gram = jnp.concatenate([gg[it, i] for i in range(ng)], axis=0)
        diagonal = jnp.sum(jnp.sum(jnp.where(eye, gram, 0.0), axis=1, keepdims=True), axis=0, keepdims=True)
        aug[:, pl.ds(0, rank)] = gram + jnp.where(eye, 1e-05 * diagonal / rank, 0.0)
        aug[:, pl.ds(rank, rank)] = jnp.where(eye, 1.0, 0.0)
        lane = lax.broadcasted_iota(jnp.int32, (PANEL, rank), 1)
        row = lax.broadcasted_iota(jnp.int32, (PANEL, 2 * rank), 0)

        def panel(p, carry):
            j = pl.multiple_of(p * PANEL, PANEL)
            lines = aug[pl.ds(j, PANEL), :]
            left = lines[:, :rank]
            heads = [
                jnp.sum(jnp.where(lane == j + i, left, 0.0), axis=1, keepdims=True) for i in range(PANEL)
            ]
            for i in range(PANEL):
                inv = lax.rsqrt(heads[i][i : i + 1, :])
                col = heads[i] * inv
                for m in range(i + 1, PANEL):
                    heads[m] = heads[m] - col * col[m : m + 1, :]
                this = lines[i : i + 1, :] * inv
                lines = jnp.where(row > i, lines - col * this, jnp.where(row == i, this, lines))
            linv[pl.ds(j, PANEL), :] = lines[:, rank:]
            aug[...] = aug[...] - outer_contract(lines[:, :rank], lines, HIGHEST)
            return carry

        lax.fori_loop(0, rank // PANEL, panel, 0)
        return linv[...] * math.sqrt(n_cells)

    for it in range(ITERS):
        order = (y_far, y_up, y_dn, my)

        def pair(n):
            for k in (ok, mk):
                g = order[n] * NK + k
                base = pl.multiple_of(g * shard, TILE)
                if it == 0:
                    residuals(g)
                part = jnp.dot(omega[...], res[:, pl.ds(base, shard)], preferred_element_type=F32)
                if k is ok:
                    psend[it, n] = part
                    out = copy(
                        psend.at[it, n], precv.at[it, n], pr_ss.at[it, n], pr_rs.at[it, n], *g_peer(my * NK + ok)
                    )
                    out.start()
                    sent.append(out)
                else:
                    pown[n] = part

        def both(n):
            copy(
                psend.at[it, n], precv.at[it, n], pr_ss.at[it, n], pr_rs.at[it, n], *g_peer(my * NK + ok)
            ).wait_recv()
            return pown[n] + precv[it, n]

        up, dn = g_peer(y_up * NK + mk), g_peer(y_dn * NK + mk)
        other = g_peer(my * NK + ok)
        top, bot = pl.ds(0, half), pl.ds(half, half)

        pair(0)
        pair(1)
        qbuf[it, 0] = both(0).astype(BF16)
        far_up = copy(qbuf.at[it, 0, top], fbuf.at[it, 0], f_ss.at[it, 0], f_rs.at[it, 0], *up)
        far_dn = copy(qbuf.at[it, 0, bot], fbuf.at[it, 1], f_ss.at[it, 1], f_rs.at[it, 1], *dn)
        far_up.start()
        far_dn.start()
        pair(2)
        q = both(1)
        far_up.wait_recv()
        qbuf[it, 1, top] = (q[:half] + fbuf[it, 0].astype(F32)).astype(BF16)
        qbuf[it, 1, bot] = q[half:].astype(BF16)
        near_up = copy(qbuf.at[it, 1], rbuf.at[it, 0], r_ss.at[it, 0], r_rs.at[it, 0], *up)
        near_up.start()
        q = both(2)
        far_dn.wait_recv()
        qbuf[it, 2, top] = q[:half].astype(BF16)
        qbuf[it, 2, bot] = (q[half:] + fbuf[it, 1].astype(F32)).astype(BF16)
        near_dn = copy(qbuf.at[it, 2], rbuf.at[it, 1], r_ss.at[it, 1], r_rs.at[it, 1], *dn)
        near_dn.start()
        pair(3)
        own = both(3)
        near_up.wait_recv()
        near_dn.wait_recv()
        sfull[it, me_g] = (own + rbuf[it, 0].astype(F32) + rbuf[it, 1].astype(F32)).astype(BF16)
        sent.extend([far_up, far_dn, near_up, near_dn])

        def block(g, part=None):
            return sfull.at[it, g] if part is None else sfull.at[it, g, part]

        def send(n, g, part, peer):
            out = copy(block(g, part), block(g, part), ag_ss.at[it, n], ag_rs.at[it, n], *peer)
            out.start()
            sent.append(out)

        def arrive(n, g, part):
            copy(block(g, part), block(g, part), ag_ss.at[it, n], ag_rs.at[it, n], *other).wait_recv()

        mine = me_g
        up_k, dn_k, far_k = (y * NK + mk for y in (y_up, y_dn, y_far))
        up_o, dn_o, far_o = (y * NK + ok for y in (y_up, y_dn, y_far))
        mine_o = my * NK + ok

        def gather(first, g):
            base = pl.multiple_of(g * shard, TILE)
            s = sfull[it, g]
            t = inner_contract(res[:, pl.ds(base, shard)], s)
            u = inner_contract(s, s)
            if first:
                tacc[it] = t
                gacc[it] = u
            else:
                tacc[it] = tacc[it] + t
                gacc[it] = gacc[it] + u

        send(0, mine, top, up)
        send(1, mine, bot, dn)
        send(2, mine, bot, up)
        send(3, mine, top, dn)
        send(4, mine, None, other)
        gather(True, mine)
        arrive(0, dn_k, top)
        send(5, dn_k, top, up)
        arrive(1, up_k, bot)
        send(6, up_k, bot, dn)
        arrive(4, mine_o, None)
        gather(False, mine_o)
        arrive(2, dn_k, bot)
        send(7, dn_k, None, other)
        arrive(3, up_k, top)
        send(8, up_k, None, other)
        gather(False, dn_k)
        gather(False, up_k)
        arrive(7, dn_o, None)
        gather(False, dn_o)
        arrive(8, up_o, None)
        gather(False, up_o)
        arrive(5, far_k, top)
        arrive(6, far_k, bot)
        send(9, far_k, None, other)
        gather(False, far_k)
        arrive(9, far_o, None)
        gather(False, far_o)
        if it == ITERS - 1:
            leave = pltpu.make_async_copy(sfull.at[it], s_out, out_sem)
            leave.start()

        for i in range(nx):
            txs[it, i] = tacc[it, pl.ds(i * blk, blk), :]
        txr[it, mx] = txs[it, mx]
        gx[it, mx] = gacc[it, pl.ds(pl.multiple_of(me_g * gr, 8), gr), :]
        got_gx = spread(nx, mx, x_peer, lambda to: gx.at[it, mx], gx.at[it], gx_ss.at[it], gx_rs.at[it])
        got_tx = spread(nx, mx, x_peer, lambda to: txs.at[it, to], txr.at[it], tx_ss.at[it], tx_rs.at[it])
        wait_all(got_gx)
        gz[it, mz] = total([gx[it, i] for i in range(nx)], nx)
        got_gz = spread(nz, mz, z_peer, lambda to: gz.at[it, mz], gz.at[it], gz_ss.at[it], gz_rs.at[it])
        wait_all(got_tx)
        tsum = total([txr[it, i] for i in range(nx)], nx)
        for i in range(nz):
            tzs[it, i] = tsum[i * zr : (i + 1) * zr, :]
        tzr[it, mz] = tzs[it, mz]
        got_tz = spread(nz, mz, z_peer, lambda to: tzs.at[it, to], tzr.at[it], tz_ss.at[it], tz_rs.at[it])
        wait_all(got_gz)
        gg[it, me_g] = total([gz[it, i] for i in range(nz)], nz)
        got_gg = spread(ng, me_g, g_peer, lambda to: gg.at[it, me_g], gg.at[it], gg_ss.at[it], gg_rs.at[it])
        wait_all(got_tz)
        tall[it, mx, mz] = total([tzr[it, i] for i in range(nz)], nz)
        got_taz = spread(
            nz, mz, z_peer, lambda to: tall.at[it, mx, mz], tall.at[it, mx], taz_ss.at[it], taz_rs.at[it]
        )
        wait_all(got_taz)
        got_tax = spread(
            nx, mx, x_peer, lambda to: tall.at[it, mx], tall.at[it], tax_ss.at[it], tax_rs.at[it]
        )
        wait_all(got_gg)
        white = whiten(it)
        if it == ITERS - 1:
            w_out[...] = white
        wait_all(got_tax)
        for i in range(nx):
            t = jnp.concatenate([tall[it, i, j] for j in range(nz)], axis=0)
            if it == ITERS - 1:
                load_out[pl.ds(i * blk, blk), :] = inner_contract(t, white, HIGHEST) * gene_scale
            else:
                omega[:, pl.ds(i * blk, blk)] = (inner_contract(white, t, HIGHEST) * gene_scale).astype(BF16)

    leave.wait()
    for s in sent:
        s.wait_send()


def shard_of(rows, ng):
    return -(-rows // (ng * TILE)) * TILE


def finish(s_ref, white_ref, load_ref, basis_ref, out_ref):
    basis_ref[...] = lax.dot_general(
        s_ref[0].astype(F32), white_ref[...], (((0,), (1,)), ((), ())), precision=HIGHEST, preferred_element_type=F32
    )
    out_ref[...] = load_ref[pl.ds(0, out_ref.shape[0]), :]


def shards(counts, sketch):
    rows, genes = counts.shape
    rank = sketch.shape[1]
    nc, ng = lax.axis_size("cells"), lax.axis_size("genes")
    nx = NX
    nz = nc // nx
    wide = -(-genes // TILE) * TILE
    shard = shard_of(rows, ng)
    blk, gr = wide // nx, rank // ng
    zr = blk // nz
    dims = (nx, nz, ng, rows, genes, wide, rank, nc * rows, ng * genes)
    V = pltpu.VMEM
    D = pltpu.SemaphoreType.DMA

    def pairs(*shape):
        return [D(shape), D(shape)]

    s_all, white, load = pl.pallas_call(
        functools.partial(kernel, dims),
        out_shape=(
            jax.ShapeDtypeStruct((ng, rank, shard), BF16),
            jax.ShapeDtypeStruct((rank, rank), F32),
            jax.ShapeDtypeStruct((wide, rank), F32),
        ),
        in_specs=[pl.BlockSpec(memory_space=pl.ANY), pl.BlockSpec(memory_space=pltpu.VMEM)],
        out_specs=(
            pl.BlockSpec(memory_space=pl.ANY),
            pl.BlockSpec(memory_space=pltpu.VMEM),
            pl.BlockSpec(memory_space=pltpu.VMEM),
        ),
        scratch_shapes=[
            V((genes, rows), jnp.int32),
            V((wide, ng * shard), BF16),
            V((genes, TILE), jnp.int32),
            V((ng, 1, rows), F32),
            V((1, rows), F32),
            V((nx, 1, wide), F32),
            V((nz, 1, wide), F32),
            V((ng, 1, TILE), F32),
            V((wide, TILE), F32),
            V((rank, wide), BF16),
            V((ITERS, 4, rank, shard), F32),
            V((ITERS, 4, rank, shard), F32),
            V((4, rank, shard), F32),
            V((ITERS, 3, rank, shard), BF16),
            V((ITERS, 2, rank // 2, shard), BF16),
            V((ITERS, 2, rank, shard), BF16),
            V((ITERS, ng, rank, shard), BF16),
            V((ITERS, wide, rank), F32),
            V((ITERS, rank, rank), F32),
            V((ITERS, nx, blk, rank), F32),
            V((ITERS, nx, blk, rank), F32),
            V((ITERS, nz, zr, rank), F32),
            V((ITERS, nz, zr, rank), F32),
            V((ITERS, nx, nz, zr, rank), F32),
            V((ITERS, nx, gr, rank), F32),
            V((ITERS, nz, gr, rank), F32),
            V((ITERS, ng, gr, rank), F32),
            V((rank, 2 * rank), F32),
            V((rank, rank), F32),
            D((rows // (PER * TILE),)),
            D,
            *pairs(nx),
            *pairs(nz),
            *pairs(ng),
            *pairs(ng),
            *pairs(ITERS, 4),
            *pairs(ITERS, 2),
            *pairs(ITERS, 2),
            *pairs(ITERS, 10),
            *pairs(ITERS, nx),
            *pairs(ITERS, nz),
            *pairs(ITERS, nz),
            *pairs(ITERS, nx),
            *pairs(ITERS, nx),
            *pairs(ITERS, nz),
            *pairs(ITERS, ng),
        ],
        compiler_params=pltpu.CompilerParams(
            collective_id=0, has_side_effects=True, vmem_limit_bytes=60 * 2**20
        ),
        name="sweep",
    )(counts.T, sketch)
    return pl.pallas_call(
        finish,
        grid=(-(-rows // shard),),
        out_shape=(
            jax.ShapeDtypeStruct((rows, rank), F32),
            jax.ShapeDtypeStruct((genes, rank), F32),
        ),
        in_specs=[
            pl.BlockSpec((1, rank, shard), lambda i: (i, 0, 0)),
            pl.BlockSpec((rank, rank), lambda i: (0, 0)),
            pl.BlockSpec((wide, rank), lambda i: (0, 0)),
        ],
        out_specs=(
            pl.BlockSpec((shard, rank), lambda i: (i, 0)),
            pl.BlockSpec((genes, rank), lambda i: (0, 0)),
        ),
        name="finish",
    )(s_all, white, load)


def solution(mesh):
    return jax.shard_map(
        shards,
        mesh=mesh,
        in_specs=(P("cells", "genes"), P("genes", None)),
        out_specs=(P("cells", None), P("genes", None)),
        check_vma=False,
    )
```

```python
import functools
import math

import jax
import jax.numpy as jnp
from jax import lax
from jax.experimental import pallas as pl
from jax.experimental.pallas import tpu as pltpu
from jax.sharding import PartitionSpec as P

ITERS = 2
NX = 4
NK = 2
TILE = 128
STEP = 32
PANEL = 8
PER = 2
BLOCKS = 4
HIGHEST = lax.Precision.HIGHEST
MESH = pl.DeviceIdType.MESH
F32 = jnp.float32
BF16 = jnp.bfloat16


def outer_contract(left, right, precision=None):
    return lax.dot_general(
        left, right, (((0,), (0,)), ((), ())), precision=precision, preferred_element_type=F32
    )


def inner_contract(left, right, precision=None):
    return lax.dot_general(
        left, right, (((1,), (1,)), ((), ())), precision=precision, preferred_element_type=F32
    )


def kernel(
    dims,
    counts_hbm,
    sketch_ref,
    s_out,
    w_out,
    load_out,
    cnt,
    res,
    gpart,
    cellx,
    totc,
    genex,
    genez,
    grp,
    fracs,
    omega,
    psend,
    precv,
    pown,
    qbuf,
    fbuf,
    rbuf,
    late,
    sfull,
    flat,
    tacc,
    gsrc,
    grow,
    txs,
    txr,
    tzs,
    tzr,
    oall,
    gx,
    gz,
    gg,
    aug,
    linv,
    load_sem,
    out_sem,
    bx_ss,
    bx_rs,
    bz_ss,
    bz_rs,
    ba_ss,
    ba_rs,
    bg_ss,
    bg_rs,
    pr_ss,
    pr_rs,
    f_ss,
    f_rs,
    ag_ss,
    ag_rs,
    tx_ss,
    tx_rs,
    tz_ss,
    tz_rs,
    taz_ss,
    taz_rs,
    tax_ss,
    tax_rs,
    gr_ss,
    gr_rs,
    gx_ss,
    gx_rs,
    gz_ss,
    gz_rs,
    gg_ss,
    gg_rs,
):
    nx, nz, ng, rows, genes, wide, rank, n_cells, n_genes = dims
    ny = ng // NK
    shard = shard_of(rows, ng)
    half, quarter = rank // 2, rank // 4
    blk = wide // nx
    zr = blk // nz
    gr = rank // ng
    me_c = lax.axis_index("cells")
    me_g = lax.axis_index("genes")
    mz, mx = me_c // nx, lax.rem(me_c, nx)
    my, mk = me_g // NK, lax.rem(me_g, NK)
    ok = 1 - mk
    y_up, y_dn, y_far = (lax.rem(my + d, ny) for d in (1, 3, 2))

    def copy(src, dst, ss, rs, c, g):
        return pltpu.make_async_remote_copy(
            src_ref=src, dst_ref=dst, send_sem=ss, recv_sem=rs, device_id=(c, g), device_id_type=MESH
        )

    def x_peer(i):
        return mz * nx + i, me_g

    def z_peer(i):
        return i * nx + mx, me_g

    def g_peer(i):
        return me_c, i

    sent = []

    def spread(n, me, peer, src_of, dst, ss, rs):
        arrivals = []
        for d in range(1, n):
            to, frm = lax.rem(me + d, n), lax.rem(me + n - d, n)
            out = copy(src_of(to), dst.at[me], ss.at[d], rs.at[d], *peer(to))
            out.start()
            sent.append(out)
            arrivals.append(copy(src_of(to), dst.at[frm], ss.at[d], rs.at[d], *peer(to)))
        return arrivals

    def wait_all(arrivals):
        for a in arrivals:
            a.wait_recv()

    def total(slots, n):
        acc = slots[0]
        for i in range(1, n):
            acc = acc + slots[i]
        return acc

    barrier = pltpu.get_barrier_semaphore()
    for n, me, peer in ((nx, mx, x_peer), (nz, mz, z_peer), (ng, me_g, g_peer)):
        for d in range(1, n):
            pl.semaphore_signal(barrier, inc=1, device_id=peer(lax.rem(me + d, n)), device_id_type=MESH)

    per = PER * TILE
    loads = rows // per

    def load(i):
        part = pl.ds(pl.multiple_of(i * per, TILE), per)
        return pltpu.make_async_copy(counts_hbm.at[:, part], cnt.at[:, part], load_sem.at[i])

    for i in range(loads):
        load(i).start()

    res[:, pl.ds(rows, ng * shard - rows)] = jnp.zeros((wide, ng * shard - rows), BF16)
    flip = jnp.transpose(sketch_ref[...].astype(F32))
    omega[...] = jnp.concatenate([flip, jnp.zeros((rank, wide - genes), F32)], axis=1).astype(BF16)
    gpart[...] = jnp.zeros((genes, TILE), jnp.int32)
    even = genes - genes % 8

    def stats(i, carry):
        load(i).wait()
        tot = None
        for j in range(PER):
            at = pl.multiple_of(i * per + j * TILE, TILE)
            x = cnt[:, pl.ds(at, TILE)]
            tot = x if tot is None else tot + x
            down = jnp.sum(x[:even].reshape(even // 8, 8, TILE), axis=0)
            down = jnp.sum(down, axis=0, keepdims=True)
            if even < genes:
                down = down + jnp.sum(x[even:], axis=0, keepdims=True)
            cellx[me_g, :, pl.ds(at, TILE)] = down.astype(F32)
        gpart[...] = gpart[...] + tot
        return carry

    lax.fori_loop(0, loads, stats, 0)
    groups = wide // TILE
    for g in range(groups):
        n = min(TILE, genes - g * TILE)
        line = gpart[pl.ds(g * TILE, n), :].astype(F32)
        if n < TILE:
            line = jnp.concatenate([line, jnp.zeros((TILE - n, TILE), F32)], axis=0)
        genex[mx, :, pl.ds(g * TILE, TILE)] = jnp.sum(jnp.transpose(line), axis=0, keepdims=True)

    pl.semaphore_wait(barrier, nx + nz + ng - 3)
    got_x = spread(nx, mx, x_peer, lambda to: genex.at[mx], genex, bx_ss, bx_rs)
    got_a = spread(ng, me_g, g_peer, lambda to: cellx.at[me_g], cellx, ba_ss, ba_rs)
    wait_all(got_x)
    genez[mz] = total(genex, nx)
    got_z = spread(nz, mz, z_peer, lambda to: genez.at[mz], genez, bz_ss, bz_rs)
    wait_all(got_a)
    totc[...] = total(cellx, ng)
    wait_all(got_z)
    gene_total = total(genez, nz)
    short = gene_total[:, :TILE]
    for g in range(1, groups):
        short = short + gene_total[:, g * TILE : (g + 1) * TILE]
    grp[me_g] = short
    got_g = spread(ng, me_g, g_peer, lambda to: grp.at[me_g], grp, bg_ss, bg_rs)
    fill = lax.broadcasted_iota(jnp.int32, (1, wide), 1) >= genes
    gene_total = jnp.where(fill, 1.0, gene_total)
    for g in range(groups):
        line = jnp.broadcast_to(gene_total[:, g * TILE : (g + 1) * TILE], (TILE, TILE))
        fracs[pl.ds(g * TILE, TILE), :] = jnp.transpose(line)
    wait_all(got_g)
    grand = jnp.sum(total(grp, ng), axis=1, keepdims=True)
    fracs[...] = fracs[...] / grand

    limit = math.sqrt(n_cells)

    def residuals(g):
        def some(t, carry):
            at = pl.ds(pl.multiple_of(t * TILE, TILE), TILE)
            cell = totc[:, at]
            for k in range(wide // STEP):
                n = min(STEP, genes - k * STEP)
                x = cnt[pl.ds(k * STEP, n), at].astype(F32)
                if n < STEP:
                    x = jnp.concatenate([x, jnp.zeros((STEP - n, TILE), F32)], axis=0)
                mu = cell * fracs[pl.ds(k * STEP, STEP), :]
                value = (x - mu) * lax.rsqrt(mu + 0.01 * mu * mu)
                value = jnp.clip(value, -limit, limit)
                if n < STEP:
                    row = lax.broadcasted_iota(jnp.int32, (STEP, TILE), 0)
                    value = jnp.where(row < n, value, 0.0)
                res[pl.ds(k * STEP, STEP), at] = value.astype(BF16)
            return carry

        first = g * (shard // TILE)
        lax.fori_loop(first, jnp.minimum(first + shard // TILE, rows // TILE), some, 0)

    gene_scale = math.sqrt(n_genes) / n_cells

    def whiten(it):
        eye = (
            lax.broadcasted_iota(jnp.int32, (rank, rank), 0)
            == lax.broadcasted_iota(jnp.int32, (rank, rank), 1)
        )
        gram = jnp.concatenate([gg[it, i] for i in range(ng)], axis=0)
        diagonal = jnp.sum(jnp.sum(jnp.where(eye, gram, 0.0), axis=1, keepdims=True), axis=0, keepdims=True)
        aug[:, pl.ds(0, rank)] = gram + jnp.where(eye, 1e-05 * diagonal / rank, 0.0)
        aug[:, pl.ds(rank, rank)] = jnp.where(eye, 1.0, 0.0)
        lane = lax.broadcasted_iota(jnp.int32, (PANEL, rank), 1)
        row = lax.broadcasted_iota(jnp.int32, (PANEL, 2 * rank), 0)

        def panel(p, carry):
            j = pl.multiple_of(p * PANEL, PANEL)
            lines = aug[pl.ds(j, PANEL), :]
            left = lines[:, :rank]
            heads = [
                jnp.sum(jnp.where(lane == j + i, left, 0.0), axis=1, keepdims=True) for i in range(PANEL)
            ]
            for i in range(PANEL):
                inv = lax.rsqrt(heads[i][i : i + 1, :])
                col = heads[i] * inv
                for m in range(i + 1, PANEL):
                    heads[m] = heads[m] - col * col[m : m + 1, :]
                this = lines[i : i + 1, :] * inv
                lines = jnp.where(row > i, lines - col * this, jnp.where(row == i, this, lines))
            linv[pl.ds(j, PANEL), :] = lines[:, rank:]
            aug[...] = aug[...] - outer_contract(lines[:, :rank], lines, HIGHEST)
            return carry

        lax.fori_loop(0, rank // PANEL, panel, 0)
        return linv[...] * math.sqrt(n_cells)

    for it in range(ITERS):
        order = (y_far, y_up, y_dn, my)

        def pair(n):
            for k in (ok, mk):
                g = order[n] * NK + k
                base = pl.multiple_of(g * shard, TILE)
                if it == 0:
                    residuals(g)
                part = jnp.dot(omega[...], res[:, pl.ds(base, shard)], preferred_element_type=F32)
                if k is ok:
                    psend[it, n] = part
                    out = copy(
                        psend.at[it, n], precv.at[it, n], pr_ss.at[it, n], pr_rs.at[it, n], *g_peer(my * NK + ok)
                    )
                    out.start()
                    sent.append(out)
                else:
                    pown[n] = part

        def both(n):
            copy(
                psend.at[it, n], precv.at[it, n], pr_ss.at[it, n], pr_rs.at[it, n], *g_peer(my * NK + ok)
            ).wait_recv()
            return pown[n] + precv[it, n]

        up, dn = g_peer(y_up * NK + mk), g_peer(y_dn * NK + mk)
        other = g_peer(my * NK + ok)
        top, bot = pl.ds(0, half), pl.ds(half, half)

        def hop(src, dst, n, peer):
            out = copy(src, dst, f_ss.at[it, n], f_rs.at[it, n], *peer)
            out.start()
            sent.append(out)
            return out

        pair(0)
        pair(1)
        qbuf[it, 0] = both(0).astype(BF16)
        far_up = hop(qbuf.at[it, 0, top], fbuf.at[it, 0], 0, up)
        far_dn = hop(qbuf.at[it, 0, bot], fbuf.at[it, 1], 1, dn)
        q = both(1)
        qbuf[it, 1, bot] = q[half:].astype(BF16)
        late[0] = q[:half]
        free_up = hop(qbuf.at[it, 1, bot], rbuf.at[it, 0, bot], 2, up)
        pair(2)
        q = both(2)
        qbuf[it, 2, top] = q[:half].astype(BF16)
        late[1] = q[half:]
        free_dn = hop(qbuf.at[it, 2, top], rbuf.at[it, 1, top], 3, dn)
        pair(3)
        far_up.wait_recv()
        qbuf[it, 1, top] = (late[0] + fbuf[it, 0].astype(F32)).astype(BF16)
        near_up = hop(qbuf.at[it, 1, top], rbuf.at[it, 0, top], 4, up)
        far_dn.wait_recv()
        qbuf[it, 2, bot] = (late[1] + fbuf[it, 1].astype(F32)).astype(BF16)
        near_dn = hop(qbuf.at[it, 2, bot], rbuf.at[it, 1, bot], 5, dn)
        own = both(3)
        for q in (free_up, free_dn, near_up, near_dn):
            q.wait_recv()
        sfull[it, me_g] = (own + rbuf[it, 0].astype(F32) + rbuf[it, 1].astype(F32)).astype(BF16)

        def block(g, first, n):
            return sfull.at[it, g, pl.ds(first * quarter, n * quarter)]

        def send(n, g, first, count, peer):
            out = copy(block(g, first, count), block(g, first, count), ag_ss.at[it, n], ag_rs.at[it, n], *peer)
            out.start()
            sent.append(out)

        def arrive(n, g, first, count):
            copy(
                block(g, first, count), block(g, first, count), ag_ss.at[it, n], ag_rs.at[it, n], *other
            ).wait_recv()

        mine = me_g
        up_k, dn_k, far_k = (y * NK + mk for y in (y_up, y_dn, y_far))
        up_o, dn_o, far_o = (y * NK + ok for y in (y_up, y_dn, y_far))
        mine_o = my * NK + ok

        def gather(first, g):
            base = pl.multiple_of(g * shard, TILE)
            t = inner_contract(res[:, pl.ds(base, shard)], sfull[it, g])
            tacc[...] = t if first else tacc[...] + t

        send(0, mine, 0, 1, up)
        send(3, mine, 2, 1, dn)
        send(1, mine, 1, 1, up)
        send(4, mine, 3, 1, dn)
        s = sfull[it, mine]
        gram = inner_contract(s, s)
        for i in range(ng):
            gsrc[it, i] = gram[i * gr : (i + 1) * gr, :]
        grow[it, me_g] = gsrc[it, me_g]
        got_gr = spread(ng, me_g, g_peer, lambda to: gsrc.at[it, to], grow.at[it], gr_ss.at[it], gr_rs.at[it])
        send(6, mine, 0, 4, other)
        send(2, mine, 2, 2, up)
        send(5, mine, 0, 2, dn)
        gather(True, mine)
        arrive(0, dn_k, 0, 1)
        send(7, dn_k, 0, 1, up)
        arrive(3, up_k, 2, 1)
        send(9, up_k, 2, 1, dn)
        arrive(1, dn_k, 1, 1)
        send(8, dn_k, 1, 1, up)
        arrive(4, up_k, 3, 1)
        send(10, up_k, 3, 1, dn)
        wait_all(got_gr)
        gx[it, mx] = total([grow[it, i] for i in range(ng)], ng)
        got_gx = spread(nx, mx, x_peer, lambda to: gx.at[it, mx], gx.at[it], gx_ss.at[it], gx_rs.at[it])
        arrive(6, mine_o, 0, 4)
        gather(False, mine_o)
        arrive(2, dn_k, 2, 2)
        send(11, dn_k, 0, 4, other)
        arrive(5, up_k, 0, 2)
        send(12, up_k, 0, 4, other)
        gather(False, dn_k)
        gather(False, up_k)
        wait_all(got_gx)
        gz[it, mz] = total([gx[it, i] for i in range(nx)], nx)
        got_gz = spread(nz, mz, z_peer, lambda to: gz.at[it, mz], gz.at[it], gz_ss.at[it], gz_rs.at[it])
        arrive(11, dn_o, 0, 4)
        gather(False, dn_o)
        arrive(7, far_k, 0, 1)
        arrive(8, far_k, 1, 1)
        send(13, far_k, 0, 2, other)
        arrive(9, far_k, 2, 1)
        arrive(10, far_k, 3, 1)
        send(14, far_k, 2, 2, other)
        arrive(12, up_o, 0, 4)
        gather(False, up_o)
        gather(False, far_k)
        arrive(13, far_o, 0, 2)
        arrive(14, far_o, 2, 2)
        gather(False, far_o)

        for i in range(nx):
            txs[it, i] = tacc[pl.ds(i * blk, blk), :].astype(BF16)
        txr[it, mx] = txs[it, mx]
        got_tx = spread(nx, mx, x_peer, lambda to: txs.at[it, to], txr.at[it], tx_ss.at[it], tx_rs.at[it])
        wait_all(got_gz)
        gg[it, me_g] = total([gz[it, i] for i in range(nz)], nz)
        got_gg = spread(ng, me_g, g_peer, lambda to: gg.at[it, me_g], gg.at[it], gg_ss.at[it], gg_rs.at[it])
        wait_all(got_tx)
        tsum = total([txr[it, i].astype(F32) for i in range(nx)], nx).astype(BF16)
        for i in range(nz):
            tzs[it, i] = tsum[i * zr : (i + 1) * zr, :]
        tzr[it, mz] = tzs[it, mz]
        got_tz = spread(nz, mz, z_peer, lambda to: tzs.at[it, to], tzr.at[it], tz_ss.at[it], tz_rs.at[it])
        wait_all(got_gg)
        white = whiten(it)
        wait_all(got_tz)
        own = inner_contract(total([tzr[it, i].astype(F32) for i in range(nz)], nz), white, HIGHEST)
        oall[it, mx, mz] = (own * gene_scale).astype(BF16)
        got_oz = spread(
            nz, mz, z_peer, lambda to: oall.at[it, mx, mz], oall.at[it, mx], taz_ss.at[it], taz_rs.at[it]
        )
        if it == ITERS - 1:
            up_front = jnp.transpose(white)
            high = up_front.astype(BF16)
            w_out[:, pl.ds(0, rank)] = high
            w_out[:, pl.ds(rank, rank)] = (up_front - high.astype(F32)).astype(BF16)
            for i in range(ng):
                flat[i] = jnp.transpose(sfull[it, i])
            leave = pltpu.make_async_copy(flat, s_out, out_sem)
            leave.start()
        wait_all(got_oz)
        got_ox = spread(
            nx, mx, x_peer, lambda to: oall.at[it, mx], oall.at[it], tax_ss.at[it], tax_rs.at[it]
        )
        wait_all(got_ox)
        for i in range(nx):
            loading = jnp.concatenate([oall[it, i, j] for j in range(nz)], axis=0)
            if it == ITERS - 1:
                load_out[pl.ds(i * blk, blk), :] = loading
            else:
                omega[:, pl.ds(i * blk, blk)] = jnp.transpose(loading)

    leave.wait()
    for s in sent:
        s.wait_send()


def shard_of(rows, ng):
    return -(-rows // (ng * TILE)) * TILE


def finish(s_ref, white_ref, load_ref, basis_ref, out_ref):
    parts = jnp.dot(s_ref[...], white_ref[...], preferred_element_type=F32)
    rank = parts.shape[1] // 2
    basis_ref[...] = parts[:, :rank] + parts[:, rank:]
    out_ref[...] = load_ref[pl.ds(0, out_ref.shape[0]), :].astype(F32)


def shards(counts, sketch):
    rows, genes = counts.shape
    rank = sketch.shape[1]
    nc, ng = lax.axis_size("cells"), lax.axis_size("genes")
    nx = NX
    nz = nc // nx
    wide = -(-genes // TILE) * TILE
    shard = shard_of(rows, ng)
    blk, gr = wide // nx, rank // ng
    zr = blk // nz
    dims = (nx, nz, ng, rows, genes, wide, rank, nc * rows, ng * genes)
    V = pltpu.VMEM
    D = pltpu.SemaphoreType.DMA

    def pairs(*shape):
        return [D(shape), D(shape)]

    s_all, white, load = pl.pallas_call(
        functools.partial(kernel, dims),
        out_shape=(
            jax.ShapeDtypeStruct((ng, shard, rank), BF16),
            jax.ShapeDtypeStruct((rank, 2 * rank), BF16),
            jax.ShapeDtypeStruct((wide, rank), BF16),
        ),
        in_specs=[pl.BlockSpec(memory_space=pl.ANY), pl.BlockSpec(memory_space=pltpu.VMEM)],
        out_specs=(
            pl.BlockSpec(memory_space=pl.ANY),
            pl.BlockSpec(memory_space=pltpu.VMEM),
            pl.BlockSpec(memory_space=pltpu.VMEM),
        ),
        scratch_shapes=[
            V((genes, rows), jnp.int32),
            V((wide, ng * shard), BF16),
            V((genes, TILE), jnp.int32),
            V((ng, 1, rows), F32),
            V((1, rows), F32),
            V((nx, 1, wide), F32),
            V((nz, 1, wide), F32),
            V((ng, 1, TILE), F32),
            V((wide, TILE), F32),
            V((rank, wide), BF16),
            V((ITERS, 4, rank, shard), F32),
            V((ITERS, 4, rank, shard), F32),
            V((4, rank, shard), F32),
            V((ITERS, 3, rank, shard), BF16),
            V((ITERS, 2, rank // 2, shard), BF16),
            V((ITERS, 2, rank, shard), BF16),
            V((2, rank // 2, shard), F32),
            V((ITERS, ng, rank, shard), BF16),
            V((ng, shard, rank), BF16),
            V((wide, rank), F32),
            V((ITERS, ng, gr, rank), F32),
            V((ITERS, ng, gr, rank), F32),
            V((ITERS, nx, blk, rank), BF16),
            V((ITERS, nx, blk, rank), BF16),
            V((ITERS, nz, zr, rank), BF16),
            V((ITERS, nz, zr, rank), BF16),
            V((ITERS, nx, nz, zr, rank), BF16),
            V((ITERS, nx, gr, rank), F32),
            V((ITERS, nz, gr, rank), F32),
            V((ITERS, ng, gr, rank), F32),
            V((rank, 2 * rank), F32),
            V((rank, rank), F32),
            D((rows // (PER * TILE),)),
            D,
            *pairs(nx),
            *pairs(nz),
            *pairs(ng),
            *pairs(ng),
            *pairs(ITERS, 4),
            *pairs(ITERS, 6),
            *pairs(ITERS, 15),
            *pairs(ITERS, nx),
            *pairs(ITERS, nz),
            *pairs(ITERS, nz),
            *pairs(ITERS, nx),
            *pairs(ITERS, ng),
            *pairs(ITERS, nx),
            *pairs(ITERS, nz),
            *pairs(ITERS, ng),
        ],
        compiler_params=pltpu.CompilerParams(
            collective_id=0, has_side_effects=True, vmem_limit_bytes=60 * 2**20
        ),
        name="sweep",
    )(counts.T, sketch)
    step = rows // BLOCKS
    return pl.pallas_call(
        finish,
        grid=(BLOCKS,),
        out_shape=(
            jax.ShapeDtypeStruct((rows, rank), F32),
            jax.ShapeDtypeStruct((genes, rank), F32),
        ),
        in_specs=[
            pl.BlockSpec((step, rank), lambda i: (i, 0)),
            pl.BlockSpec((rank, 2 * rank), lambda i: (0, 0)),
            pl.BlockSpec((wide, rank), lambda i: (0, 0)),
        ],
        out_specs=(
            pl.BlockSpec((step, rank), lambda i: (i, 0)),
            pl.BlockSpec((genes, rank), lambda i: (0, 0)),
        ),
        name="finish",
    )(s_all.reshape(ng * shard, rank), white, load)


def solution(mesh):
    return jax.shard_map(
        shards,
        mesh=mesh,
        in_specs=(P("cells", "genes"), P("genes", None)),
        out_specs=(P("cells", None), P("genes", None)),
        check_vma=False,
    )
```

```python
import functools
import math

import jax
import jax.numpy as jnp
from jax import lax
from jax.experimental import pallas as pl
from jax.experimental.pallas import tpu as pltpu
from jax.sharding import PartitionSpec as P

ITERS = 2
NX = 4
NK = 2
TILE = 128
STEP = 32
PANEL = 8
PER = 2
BLOCKS = 4
HIGHEST = lax.Precision.HIGHEST
MESH = pl.DeviceIdType.MESH
F32 = jnp.float32
BF16 = jnp.bfloat16


def outer_contract(left, right, precision=None):
    return lax.dot_general(
        left, right, (((0,), (0,)), ((), ())), precision=precision, preferred_element_type=F32
    )


def inner_contract(left, right, precision=None):
    return lax.dot_general(
        left, right, (((1,), (1,)), ((), ())), precision=precision, preferred_element_type=F32
    )


def kernel(
    dims,
    counts_hbm,
    sketch_ref,
    s_out,
    w_out,
    load_out,
    cnt,
    res,
    gpart,
    cellx,
    totc,
    genex,
    genez,
    grp,
    fracs,
    omega,
    psend,
    precv,
    pown,
    qbuf,
    fbuf,
    rbuf,
    late,
    sfull,
    flat,
    tacc,
    gsrc,
    grow,
    short_s,
    short_r,
    short_all,
    wide_s,
    wide_r,
    wide_all,
    tzs,
    tzr,
    halves,
    gx,
    gz,
    gg,
    aug,
    linv,
    load_sem,
    out_sem,
    bx_ss,
    bx_rs,
    bz_ss,
    bz_rs,
    ba_ss,
    ba_rs,
    bg_ss,
    bg_rs,
    pr_ss,
    pr_rs,
    f_ss,
    f_rs,
    ag_ss,
    ag_rs,
    tx_ss,
    tx_rs,
    tz_ss,
    tz_rs,
    taz_ss,
    taz_rs,
    tax_ss,
    tax_rs,
    gr_ss,
    gr_rs,
    gx_ss,
    gx_rs,
    gz_ss,
    gz_rs,
    gg_ss,
    gg_rs,
):
    nx, nz, ng, rows, genes, wide, rank, n_cells, n_genes = dims
    ny = ng // NK
    shard = shard_of(rows, ng)
    half, quarter = rank // 2, rank // 4
    blk = wide // nx
    zr = blk // nz
    gr = rank // ng
    me_c = lax.axis_index("cells")
    me_g = lax.axis_index("genes")
    mz, mx = me_c // nx, lax.rem(me_c, nx)
    my, mk = me_g // NK, lax.rem(me_g, NK)
    ok = 1 - mk
    y_up, y_dn, y_far = (lax.rem(my + d, ny) for d in (1, 3, 2))

    def copy(src, dst, ss, rs, c, g):
        return pltpu.make_async_remote_copy(
            src_ref=src, dst_ref=dst, send_sem=ss, recv_sem=rs, device_id=(c, g), device_id_type=MESH
        )

    def x_peer(i):
        return mz * nx + i, me_g

    def z_peer(i):
        return i * nx + mx, me_g

    def g_peer(i):
        return me_c, i

    sent = []

    def spread(n, me, peer, src_of, dst, ss, rs):
        arrivals = []
        for d in range(1, n):
            to, frm = lax.rem(me + d, n), lax.rem(me + n - d, n)
            out = copy(src_of(to), dst.at[me], ss.at[d], rs.at[d], *peer(to))
            out.start()
            sent.append(out)
            arrivals.append(copy(src_of(to), dst.at[frm], ss.at[d], rs.at[d], *peer(to)))
        return arrivals

    def wait_all(arrivals):
        for a in arrivals:
            a.wait_recv()

    def total(slots, n):
        acc = slots[0]
        for i in range(1, n):
            acc = acc + slots[i]
        return acc

    barrier = pltpu.get_barrier_semaphore()
    for n, me, peer in ((nx, mx, x_peer), (nz, mz, z_peer), (ng, me_g, g_peer)):
        for d in range(1, n):
            pl.semaphore_signal(barrier, inc=1, device_id=peer(lax.rem(me + d, n)), device_id_type=MESH)

    per = PER * TILE
    loads = rows // per

    def load(i):
        part = pl.ds(pl.multiple_of(i * per, TILE), per)
        return pltpu.make_async_copy(counts_hbm.at[:, part], cnt.at[:, part], load_sem.at[i])

    for i in range(loads):
        load(i).start()

    res[:, pl.ds(rows, ng * shard - rows)] = jnp.zeros((wide, ng * shard - rows), BF16)
    flip = jnp.transpose(sketch_ref[...].astype(F32))
    omega[...] = jnp.concatenate([flip, jnp.zeros((rank, wide - genes), F32)], axis=1).astype(BF16)
    gpart[...] = jnp.zeros((genes, TILE), jnp.int32)
    even = genes - genes % 8

    def stats(i, carry):
        load(i).wait()
        tot = None
        for j in range(PER):
            at = pl.multiple_of(i * per + j * TILE, TILE)
            x = cnt[:, pl.ds(at, TILE)]
            tot = x if tot is None else tot + x
            down = jnp.sum(x[:even].reshape(even // 8, 8, TILE), axis=0)
            down = jnp.sum(down, axis=0, keepdims=True)
            if even < genes:
                down = down + jnp.sum(x[even:], axis=0, keepdims=True)
            cellx[me_g, :, pl.ds(at, TILE)] = down.astype(F32)
        gpart[...] = gpart[...] + tot
        return carry

    lax.fori_loop(0, loads, stats, 0)
    groups = wide // TILE
    for g in range(groups):
        n = min(TILE, genes - g * TILE)
        line = gpart[pl.ds(g * TILE, n), :].astype(F32)
        if n < TILE:
            line = jnp.concatenate([line, jnp.zeros((TILE - n, TILE), F32)], axis=0)
        genex[mx, :, pl.ds(g * TILE, TILE)] = jnp.sum(jnp.transpose(line), axis=0, keepdims=True)

    pl.semaphore_wait(barrier, nx + nz + ng - 3)
    got_x = spread(nx, mx, x_peer, lambda to: genex.at[mx], genex, bx_ss, bx_rs)
    got_a = spread(ng, me_g, g_peer, lambda to: cellx.at[me_g], cellx, ba_ss, ba_rs)
    wait_all(got_x)
    genez[mz] = total(genex, nx)
    got_z = spread(nz, mz, z_peer, lambda to: genez.at[mz], genez, bz_ss, bz_rs)
    wait_all(got_a)
    totc[...] = total(cellx, ng)
    wait_all(got_z)
    gene_total = total(genez, nz)
    short = gene_total[:, :TILE]
    for g in range(1, groups):
        short = short + gene_total[:, g * TILE : (g + 1) * TILE]
    grp[me_g] = short
    got_g = spread(ng, me_g, g_peer, lambda to: grp.at[me_g], grp, bg_ss, bg_rs)
    fill = lax.broadcasted_iota(jnp.int32, (1, wide), 1) >= genes
    gene_total = jnp.where(fill, 1.0, gene_total)
    for g in range(groups):
        line = jnp.broadcast_to(gene_total[:, g * TILE : (g + 1) * TILE], (TILE, TILE))
        fracs[pl.ds(g * TILE, TILE), :] = jnp.transpose(line)
    wait_all(got_g)
    grand = jnp.sum(total(grp, ng), axis=1, keepdims=True)
    fracs[...] = fracs[...] / grand

    limit = math.sqrt(n_cells)

    def residuals(g):
        def some(t, carry):
            at = pl.ds(pl.multiple_of(t * TILE, TILE), TILE)
            cell = totc[:, at]
            for k in range(wide // STEP):
                n = min(STEP, genes - k * STEP)
                x = cnt[pl.ds(k * STEP, n), at].astype(F32)
                if n < STEP:
                    x = jnp.concatenate([x, jnp.zeros((STEP - n, TILE), F32)], axis=0)
                mu = cell * fracs[pl.ds(k * STEP, STEP), :]
                value = (x - mu) * lax.rsqrt(mu + 0.01 * mu * mu)
                value = jnp.clip(value, -limit, limit)
                if n < STEP:
                    row = lax.broadcasted_iota(jnp.int32, (STEP, TILE), 0)
                    value = jnp.where(row < n, value, 0.0)
                res[pl.ds(k * STEP, STEP), at] = value.astype(BF16)
            return carry

        first = g * (shard // TILE)
        lax.fori_loop(first, jnp.minimum(first + shard // TILE, rows // TILE), some, 0)

    gene_scale = math.sqrt(n_genes) / n_cells
    shorts, wides = (short_s, short_r, short_all), (wide_s, wide_r, wide_all)

    def shift_gram(it):
        eye = (
            lax.broadcasted_iota(jnp.int32, (rank, rank), 0)
            == lax.broadcasted_iota(jnp.int32, (rank, rank), 1)
        )
        gram = jnp.concatenate([gg[it, i] for i in range(ng)], axis=0)
        diagonal = jnp.sum(jnp.sum(jnp.where(eye, gram, 0.0), axis=1, keepdims=True), axis=0, keepdims=True)
        aug[:, pl.ds(0, rank)] = gram + jnp.where(eye, 1e-05 * diagonal / rank, 0.0)
        aug[:, pl.ds(rank, rank)] = jnp.where(eye, 1.0, 0.0)

    def panels(first, last):
        lane = lax.broadcasted_iota(jnp.int32, (PANEL, rank), 1)
        row = lax.broadcasted_iota(jnp.int32, (PANEL, 2 * rank), 0)

        def panel(p, carry):
            j = pl.multiple_of(p * PANEL, PANEL)
            lines = aug[pl.ds(j, PANEL), :]
            left = lines[:, :rank]
            heads = [
                jnp.sum(jnp.where(lane == j + i, left, 0.0), axis=1, keepdims=True) for i in range(PANEL)
            ]
            for i in range(PANEL):
                inv = lax.rsqrt(heads[i][i : i + 1, :])
                col = heads[i] * inv
                for m in range(i + 1, PANEL):
                    heads[m] = heads[m] - col * col[m : m + 1, :]
                this = lines[i : i + 1, :] * inv
                lines = jnp.where(row > i, lines - col * this, jnp.where(row == i, this, lines))
            linv[pl.ds(j, PANEL), :] = lines[:, rank:]
            aug[...] = aug[...] - outer_contract(lines[:, :rank], lines, HIGHEST)
            return carry

        lax.fori_loop(first, last, panel, 0)

    for it in range(ITERS):
        order = (y_far, y_up, y_dn, my)

        def pair(n):
            for k in (ok, mk):
                g = order[n] * NK + k
                base = pl.multiple_of(g * shard, TILE)
                if it == 0:
                    residuals(g)
                part = jnp.dot(omega[...], res[:, pl.ds(base, shard)], preferred_element_type=F32)
                if k is ok:
                    psend[it, n] = part
                    out = copy(
                        psend.at[it, n], precv.at[it, n], pr_ss.at[it, n], pr_rs.at[it, n], *g_peer(my * NK + ok)
                    )
                    out.start()
                    sent.append(out)
                else:
                    pown[n] = part

        def both(n):
            copy(
                psend.at[it, n], precv.at[it, n], pr_ss.at[it, n], pr_rs.at[it, n], *g_peer(my * NK + ok)
            ).wait_recv()
            return pown[n] + precv[it, n]

        up, dn = g_peer(y_up * NK + mk), g_peer(y_dn * NK + mk)
        other = g_peer(my * NK + ok)
        top, bot = pl.ds(0, half), pl.ds(half, half)

        def hop(src, dst, n, peer):
            out = copy(src, dst, f_ss.at[it, n], f_rs.at[it, n], *peer)
            out.start()
            sent.append(out)
            return out

        pair(0)
        pair(1)
        qbuf[it, 0] = both(0).astype(BF16)
        far_up = hop(qbuf.at[it, 0, top], fbuf.at[it, 0], 0, up)
        far_dn = hop(qbuf.at[it, 0, bot], fbuf.at[it, 1], 1, dn)
        q = both(1)
        qbuf[it, 1, bot] = q[half:].astype(BF16)
        late[0] = q[:half]
        free_up = hop(qbuf.at[it, 1, bot], rbuf.at[it, 0, bot], 2, up)
        pair(2)
        q = both(2)
        qbuf[it, 2, top] = q[:half].astype(BF16)
        late[1] = q[half:]
        free_dn = hop(qbuf.at[it, 2, top], rbuf.at[it, 1, top], 3, dn)
        pair(3)
        far_up.wait_recv()
        qbuf[it, 1, top] = (late[0] + fbuf[it, 0].astype(F32)).astype(BF16)
        near_up = hop(qbuf.at[it, 1, top], rbuf.at[it, 0, top], 4, up)
        far_dn.wait_recv()
        qbuf[it, 2, bot] = (late[1] + fbuf[it, 1].astype(F32)).astype(BF16)
        near_dn = hop(qbuf.at[it, 2, bot], rbuf.at[it, 1, bot], 5, dn)
        own = both(3)
        for q in (free_up, free_dn, near_up, near_dn):
            q.wait_recv()
        sfull[it, me_g] = (own + rbuf[it, 0].astype(F32) + rbuf[it, 1].astype(F32)).astype(BF16)

        def block(g, first, n):
            return sfull.at[it, g, pl.ds(first * quarter, n * quarter)]

        def send(n, g, first, count, peer):
            out = copy(block(g, first, count), block(g, first, count), ag_ss.at[it, n], ag_rs.at[it, n], *peer)
            out.start()
            sent.append(out)

        def arrive(n, g, first, count):
            copy(
                block(g, first, count), block(g, first, count), ag_ss.at[it, n], ag_rs.at[it, n], *other
            ).wait_recv()

        mine = me_g
        up_k, dn_k, far_k = (y * NK + mk for y in (y_up, y_dn, y_far))
        up_o, dn_o, far_o = (y * NK + ok for y in (y_up, y_dn, y_far))
        mine_o = my * NK + ok

        def gather(first, g):
            base = pl.multiple_of(g * shard, TILE)
            t = inner_contract(res[:, pl.ds(base, shard)], sfull[it, g])
            tacc[...] = t if first else tacc[...] + t

        send(0, mine, 0, 1, up)
        send(3, mine, 2, 1, dn)
        send(1, mine, 1, 1, up)
        send(4, mine, 3, 1, dn)
        s = sfull[it, mine]
        gram = inner_contract(s, s)
        for i in range(ng):
            gsrc[it, i] = gram[i * gr : (i + 1) * gr, :]
        grow[it, me_g] = gsrc[it, me_g]
        got_gr = spread(ng, me_g, g_peer, lambda to: gsrc.at[it, to], grow.at[it], gr_ss.at[it], gr_rs.at[it])
        send(6, mine, 0, 4, other)
        send(2, mine, 2, 2, up)
        send(5, mine, 0, 2, dn)
        gather(True, mine)
        arrive(0, dn_k, 0, 1)
        send(7, dn_k, 0, 1, up)
        arrive(3, up_k, 2, 1)
        send(9, up_k, 2, 1, dn)
        arrive(1, dn_k, 1, 1)
        send(8, dn_k, 1, 1, up)
        arrive(4, up_k, 3, 1)
        send(10, up_k, 3, 1, dn)
        wait_all(got_gr)
        gx[it, mx] = total([grow[it, i] for i in range(ng)], ng)
        got_gx = spread(nx, mx, x_peer, lambda to: gx.at[it, mx], gx.at[it], gx_ss.at[it], gx_rs.at[it])
        arrive(6, mine_o, 0, 4)
        gather(False, mine_o)
        arrive(2, dn_k, 2, 2)
        send(11, dn_k, 0, 4, other)
        arrive(5, up_k, 0, 2)
        send(12, up_k, 0, 4, other)
        gather(False, dn_k)
        gather(False, up_k)
        wait_all(got_gx)
        gz[it, mz] = total([gx[it, i] for i in range(nx)], nx)
        got_gz = spread(nz, mz, z_peer, lambda to: gz.at[it, mz], gz.at[it], gz_ss.at[it], gz_rs.at[it])
        arrive(11, dn_o, 0, 4)
        gather(False, dn_o)
        arrive(7, far_k, 0, 1)
        arrive(8, far_k, 1, 1)
        send(13, far_k, 0, 2, other)
        arrive(9, far_k, 2, 1)
        arrive(10, far_k, 3, 1)
        send(14, far_k, 2, 2, other)
        arrive(12, up_o, 0, 4)
        gather(False, up_o)
        gather(False, far_k)
        arrive(13, far_o, 0, 2)
        arrive(14, far_o, 2, 2)
        gather(False, far_o)

        txs, txr, tall = wides if it == ITERS - 1 else shorts
        for i in range(nx):
            txs[i] = tacc[pl.ds(i * blk, blk), :].astype(txs.dtype)
        txr[mx] = txs[mx]
        got_tx = spread(nx, mx, x_peer, lambda to: txs.at[to], txr, tx_ss.at[it], tx_rs.at[it])
        wait_all(got_gz)
        gg[it, me_g] = total([gz[it, i] for i in range(nz)], nz)
        got_gg = spread(ng, me_g, g_peer, lambda to: gg.at[it, me_g], gg.at[it], gg_ss.at[it], gg_rs.at[it])
        wait_all(got_tx)
        tsum = total([txr[i].astype(F32) for i in range(nx)], nx)
        for i in range(nz):
            tzs[it, i] = tsum[i * zr : (i + 1) * zr, :]
        tzr[it, mz] = tzs[it, mz]
        got_tz = spread(nz, mz, z_peer, lambda to: tzs.at[it, to], tzr.at[it], tz_ss.at[it], tz_rs.at[it])
        if it == ITERS - 1:
            for i in range(ng):
                flat[i] = jnp.transpose(sfull[it, i])
            leave = pltpu.make_async_copy(flat, s_out, out_sem)
            leave.start()
        wait_all(got_tz)
        tall[mx, mz] = total([tzr[it, i] for i in range(nz)], nz).astype(tall.dtype)
        got_taz = spread(
            nz, mz, z_peer, lambda to: tall.at[mx, mz], tall.at[mx], taz_ss.at[it], taz_rs.at[it]
        )
        wait_all(got_gg)
        shift_gram(it)
        panels(0, rank // PANEL * 5 // 8)
        wait_all(got_taz)
        got_tax = spread(
            nx, mx, x_peer, lambda to: tall.at[mx], tall, tax_ss.at[it], tax_rs.at[it]
        )
        panels(rank // PANEL * 5 // 8, rank // PANEL)
        white = linv[...] * math.sqrt(n_cells)
        front = jnp.transpose(white) if it == ITERS - 1 else white
        high = front.astype(BF16)
        low = (front - high.astype(F32)).astype(BF16)
        if it == ITERS - 1:
            w_out[:, pl.ds(0, rank)] = high
            w_out[:, pl.ds(rank, rank)] = low
        else:
            halves[pl.ds(0, rank), :] = high
            halves[pl.ds(rank, rank), :] = low
        wait_all(got_tax)
        for i in range(nx):
            t = jnp.concatenate([tall[i, j] for j in range(nz)], axis=0)
            if it == ITERS - 1:
                load_out[pl.ds(i * blk, blk), :] = inner_contract(t, white, HIGHEST) * gene_scale
            else:
                flip = inner_contract(halves[...], t)
                omega[:, pl.ds(i * blk, blk)] = ((flip[:rank] + flip[rank:]) * gene_scale).astype(BF16)

    leave.wait()
    for s in sent:
        s.wait_send()


def shard_of(rows, ng):
    return -(-rows // (ng * TILE)) * TILE


def finish(s_ref, white_ref, load_ref, basis_ref, out_ref):
    parts = jnp.dot(s_ref[...], white_ref[...], preferred_element_type=F32)
    rank = parts.shape[1] // 2
    basis_ref[...] = parts[:, :rank] + parts[:, rank:]
    out_ref[...] = load_ref[pl.ds(0, out_ref.shape[0]), :]


def shards(counts, sketch):
    rows, genes = counts.shape
    rank = sketch.shape[1]
    nc, ng = lax.axis_size("cells"), lax.axis_size("genes")
    nx = NX
    nz = nc // nx
    wide = -(-genes // TILE) * TILE
    shard = shard_of(rows, ng)
    blk, gr = wide // nx, rank // ng
    zr = blk // nz
    dims = (nx, nz, ng, rows, genes, wide, rank, nc * rows, ng * genes)
    V = pltpu.VMEM
    D = pltpu.SemaphoreType.DMA

    def pairs(*shape):
        return [D(shape), D(shape)]

    s_all, white, load = pl.pallas_call(
        functools.partial(kernel, dims),
        out_shape=(
            jax.ShapeDtypeStruct((ng, shard, rank), BF16),
            jax.ShapeDtypeStruct((rank, 2 * rank), BF16),
            jax.ShapeDtypeStruct((wide, rank), F32),
        ),
        in_specs=[pl.BlockSpec(memory_space=pl.ANY), pl.BlockSpec(memory_space=pltpu.VMEM)],
        out_specs=(
            pl.BlockSpec(memory_space=pl.ANY),
            pl.BlockSpec(memory_space=pltpu.VMEM),
            pl.BlockSpec(memory_space=pltpu.VMEM),
        ),
        scratch_shapes=[
            V((genes, rows), jnp.int32),
            V((wide, ng * shard), BF16),
            V((genes, TILE), jnp.int32),
            V((ng, 1, rows), F32),
            V((1, rows), F32),
            V((nx, 1, wide), F32),
            V((nz, 1, wide), F32),
            V((ng, 1, TILE), F32),
            V((wide, TILE), F32),
            V((rank, wide), BF16),
            V((ITERS, 4, rank, shard), F32),
            V((ITERS, 4, rank, shard), F32),
            V((4, rank, shard), F32),
            V((ITERS, 3, rank, shard), BF16),
            V((ITERS, 2, rank // 2, shard), BF16),
            V((ITERS, 2, rank, shard), BF16),
            V((2, rank // 2, shard), F32),
            V((ITERS, ng, rank, shard), BF16),
            V((ng, shard, rank), BF16),
            V((wide, rank), F32),
            V((ITERS, ng, gr, rank), F32),
            V((ITERS, ng, gr, rank), F32),
            V((nx, blk, rank), BF16),
            V((nx, blk, rank), BF16),
            V((nx, nz, zr, rank), BF16),
            V((nx, blk, rank), F32),
            V((nx, blk, rank), F32),
            V((nx, nz, zr, rank), F32),
            V((ITERS, nz, zr, rank), F32),
            V((ITERS, nz, zr, rank), F32),
            V((2 * rank, rank), BF16),
            V((ITERS, nx, gr, rank), F32),
            V((ITERS, nz, gr, rank), F32),
            V((ITERS, ng, gr, rank), F32),
            V((rank, 2 * rank), F32),
            V((rank, rank), F32),
            D((rows // (PER * TILE),)),
            D,
            *pairs(nx),
            *pairs(nz),
            *pairs(ng),
            *pairs(ng),
            *pairs(ITERS, 4),
            *pairs(ITERS, 6),
            *pairs(ITERS, 15),
            *pairs(ITERS, nx),
            *pairs(ITERS, nz),
            *pairs(ITERS, nz),
            *pairs(ITERS, nx),
            *pairs(ITERS, ng),
            *pairs(ITERS, nx),
            *pairs(ITERS, nz),
            *pairs(ITERS, ng),
        ],
        compiler_params=pltpu.CompilerParams(
            collective_id=0, has_side_effects=True, vmem_limit_bytes=60 * 2**20
        ),
        name="sweep",
    )(counts.T, sketch)
    step = rows // BLOCKS
    return pl.pallas_call(
        finish,
        grid=(BLOCKS,),
        out_shape=(
            jax.ShapeDtypeStruct((rows, rank), F32),
            jax.ShapeDtypeStruct((genes, rank), F32),
        ),
        in_specs=[
            pl.BlockSpec((step, rank), lambda i: (i, 0)),
            pl.BlockSpec((rank, 2 * rank), lambda i: (0, 0)),
            pl.BlockSpec((wide, rank), lambda i: (0, 0)),
        ],
        out_specs=(
            pl.BlockSpec((step, rank), lambda i: (i, 0)),
            pl.BlockSpec((genes, rank), lambda i: (0, 0)),
        ),
        name="finish",
    )(s_all.reshape(ng * shard, rank), white, load)


def solution(mesh):
    return jax.shard_map(
        shards,
        mesh=mesh,
        in_specs=(P("cells", "genes"), P("genes", None)),
        out_specs=(P("cells", None), P("genes", None)),
        check_vma=False,
    )
```

```python
import functools
import math

import jax
import jax.numpy as jnp
from jax import lax
from jax.experimental import pallas as pl
from jax.experimental.pallas import tpu as pltpu
from jax.sharding import PartitionSpec as P

ITERS = 2
NX = 4
NK = 2
TILE = 128
STEP = 32
PANEL = 8
PER = 2
BLOCKS = 2
HIGHEST = lax.Precision.HIGHEST
MESH = pl.DeviceIdType.MESH
F32 = jnp.float32
BF16 = jnp.bfloat16


def outer_contract(left, right, precision=None):
    return lax.dot_general(
        left, right, (((0,), (0,)), ((), ())), precision=precision, preferred_element_type=F32
    )


def inner_contract(left, right, precision=None):
    return lax.dot_general(
        left, right, (((1,), (1,)), ((), ())), precision=precision, preferred_element_type=F32
    )


def kernel(
    dims,
    counts_hbm,
    sketch_ref,
    s_out,
    w_out,
    load_out,
    cnt,
    res,
    gpart,
    cellx,
    totc,
    genec,
    grp,
    fracs,
    omega,
    psend,
    precv,
    pown,
    qbuf,
    fbuf,
    rbuf,
    late,
    sfull,
    flat,
    tacc,
    gsrc,
    grow,
    short_s,
    short_r,
    short_all,
    wide_s,
    wide_r,
    wide_all,
    tzs,
    tzr,
    halves,
    gx,
    gz,
    gg,
    aug,
    linv,
    load_sem,
    out_sem,
    bx_ss,
    bx_rs,
    ba_ss,
    ba_rs,
    bg_ss,
    bg_rs,
    pr_ss,
    pr_rs,
    f_ss,
    f_rs,
    ag_ss,
    ag_rs,
    dr_ss,
    dr_rs,
    da_ss,
    da_rs,
    tx_ss,
    tx_rs,
    tz_ss,
    tz_rs,
    taz_ss,
    taz_rs,
    tax_ss,
    tax_rs,
    gr_ss,
    gr_rs,
    gx_ss,
    gx_rs,
    gz_ss,
    gz_rs,
    gg_ss,
    gg_rs,
):
    nx, nz, ng, rows, genes, wide, rank, n_cells, n_genes = dims
    ny = ng // NK
    nc = nx * nz
    shard = shard_of(rows, ng)
    half, quarter = rank // 2, rank // 4
    blk = wide // nx
    zr = blk // nz
    gr = rank // ng
    me_c = lax.axis_index("cells")
    me_g = lax.axis_index("genes")
    mz, mx = me_c // nx, lax.rem(me_c, nx)
    my, mk = me_g // NK, lax.rem(me_g, NK)
    ok = 1 - mk
    y_up, y_dn, y_far = (lax.rem(my + d, ny) for d in (1, 3, 2))

    def copy(src, dst, ss, rs, c, g):
        return pltpu.make_async_remote_copy(
            src_ref=src, dst_ref=dst, send_sem=ss, recv_sem=rs, device_id=(c, g), device_id_type=MESH
        )

    def c_peer(i):
        return i, me_g

    def x_peer(i):
        return mz * nx + i, me_g

    def z_peer(i):
        return i * nx + mx, me_g

    def g_peer(i):
        return me_c, i

    sent = []

    def spread(n, me, peer, src_of, dst, ss, rs):
        arrivals = []
        for d in range(1, n):
            to, frm = lax.rem(me + d, n), lax.rem(me + n - d, n)
            out = copy(src_of(to), dst.at[me], ss.at[d], rs.at[d], *peer(to))
            out.start()
            sent.append(out)
            arrivals.append(copy(src_of(to), dst.at[frm], ss.at[d], rs.at[d], *peer(to)))
        return arrivals

    def wait_all(arrivals):
        for a in arrivals:
            a.wait_recv()

    def total(slots, n):
        acc = slots[0]
        for i in range(1, n):
            acc = acc + slots[i]
        return acc

    barrier = pltpu.get_barrier_semaphore()
    for n, me, peer in ((nc, me_c, c_peer), (ng, me_g, g_peer)):
        for d in range(1, n):
            pl.semaphore_signal(barrier, inc=1, device_id=peer(lax.rem(me + d, n)), device_id_type=MESH)

    per = PER * TILE
    loads = rows // per

    def load(i):
        part = pl.ds(pl.multiple_of(i * per, TILE), per)
        return pltpu.make_async_copy(counts_hbm.at[:, part], cnt.at[:, part], load_sem.at[i])

    for i in range(loads):
        load(i).start()

    res[:, pl.ds(rows, ng * shard - rows)] = jnp.zeros((wide, ng * shard - rows), BF16)
    flip = jnp.transpose(sketch_ref[...].astype(F32))
    omega[...] = jnp.concatenate([flip, jnp.zeros((rank, wide - genes), F32)], axis=1).astype(BF16)
    gpart[...] = jnp.zeros((genes, TILE), jnp.int32)
    even = genes - genes % 8

    def stats(i, carry):
        load(i).wait()
        tot = None
        for j in range(PER):
            at = pl.multiple_of(i * per + j * TILE, TILE)
            x = cnt[:, pl.ds(at, TILE)]
            tot = x if tot is None else tot + x
            down = jnp.sum(x[:even].reshape(even // 8, 8, TILE), axis=0)
            down = jnp.sum(down, axis=0, keepdims=True)
            if even < genes:
                down = down + jnp.sum(x[even:], axis=0, keepdims=True)
            cellx[me_g, :, pl.ds(at, TILE)] = down.astype(F32)
        gpart[...] = gpart[...] + tot
        return carry

    lax.fori_loop(0, loads, stats, 0)
    groups = wide // TILE
    for g in range(groups):
        n = min(TILE, genes - g * TILE)
        line = gpart[pl.ds(g * TILE, n), :].astype(F32)
        if n < TILE:
            line = jnp.concatenate([line, jnp.zeros((TILE - n, TILE), F32)], axis=0)
        genec[me_c, :, pl.ds(g * TILE, TILE)] = jnp.sum(jnp.transpose(line), axis=0, keepdims=True)

    pl.semaphore_wait(barrier, nc + ng - 2)
    got_c = spread(nc, me_c, c_peer, lambda to: genec.at[me_c], genec, bx_ss, bx_rs)
    got_a = spread(ng, me_g, g_peer, lambda to: cellx.at[me_g], cellx, ba_ss, ba_rs)
    wait_all(got_a)
    totc[...] = total(cellx, ng)
    wait_all(got_c)
    gene_total = total(genec, nc)
    short = gene_total[:, :TILE]
    for g in range(1, groups):
        short = short + gene_total[:, g * TILE : (g + 1) * TILE]
    grp[me_g] = short
    got_g = spread(ng, me_g, g_peer, lambda to: grp.at[me_g], grp, bg_ss, bg_rs)
    fill = lax.broadcasted_iota(jnp.int32, (1, wide), 1) >= genes
    gene_total = jnp.where(fill, 1.0, gene_total)
    for g in range(groups):
        line = jnp.broadcast_to(gene_total[:, g * TILE : (g + 1) * TILE], (TILE, TILE))
        fracs[pl.ds(g * TILE, TILE), :] = jnp.transpose(line)
    wait_all(got_g)
    grand = jnp.sum(total(grp, ng), axis=1, keepdims=True)
    fracs[...] = fracs[...] / grand

    limit = math.sqrt(n_cells)

    def residuals(g):
        def some(t, carry):
            at = pl.ds(pl.multiple_of(t * TILE, TILE), TILE)
            cell = totc[:, at]
            for k in range(wide // STEP):
                n = min(STEP, genes - k * STEP)
                x = cnt[pl.ds(k * STEP, n), at].astype(F32)
                if n < STEP:
                    x = jnp.concatenate([x, jnp.zeros((STEP - n, TILE), F32)], axis=0)
                mu = cell * fracs[pl.ds(k * STEP, STEP), :]
                value = (x - mu) * lax.rsqrt(mu + 0.01 * mu * mu)
                value = jnp.clip(value, -limit, limit)
                if n < STEP:
                    row = lax.broadcasted_iota(jnp.int32, (STEP, TILE), 0)
                    value = jnp.where(row < n, value, 0.0)
                res[pl.ds(k * STEP, STEP), at] = value.astype(BF16)
            return carry

        first = g * (shard // TILE)
        lax.fori_loop(first, jnp.minimum(first + shard // TILE, rows // TILE), some, 0)

    gene_scale = math.sqrt(n_genes) / n_cells
    piece = wide // nc

    def shift_gram(it):
        eye = (
            lax.broadcasted_iota(jnp.int32, (rank, rank), 0)
            == lax.broadcasted_iota(jnp.int32, (rank, rank), 1)
        )
        gram = jnp.concatenate([gg[it, i] for i in range(ng)], axis=0)
        diagonal = jnp.sum(jnp.sum(jnp.where(eye, gram, 0.0), axis=1, keepdims=True), axis=0, keepdims=True)
        aug[:, pl.ds(0, rank)] = gram + jnp.where(eye, 1e-05 * diagonal / rank, 0.0)
        aug[:, pl.ds(rank, rank)] = jnp.where(eye, 1.0, 0.0)

    def panels(first, last):
        lane = lax.broadcasted_iota(jnp.int32, (PANEL, rank), 1)
        row = lax.broadcasted_iota(jnp.int32, (PANEL, 2 * rank), 0)

        def panel(p, carry):
            j = pl.multiple_of(p * PANEL, PANEL)
            lines = aug[pl.ds(j, PANEL), :]
            left = lines[:, :rank]
            heads = [
                jnp.sum(jnp.where(lane == j + i, left, 0.0), axis=1, keepdims=True) for i in range(PANEL)
            ]
            for i in range(PANEL):
                inv = lax.rsqrt(heads[i][i : i + 1, :])
                col = heads[i] * inv
                for m in range(i + 1, PANEL):
                    heads[m] = heads[m] - col * col[m : m + 1, :]
                this = lines[i : i + 1, :] * inv
                lines = jnp.where(row > i, lines - col * this, jnp.where(row == i, this, lines))
            linv[pl.ds(j, PANEL), :] = lines[:, rank:]
            aug[...] = aug[...] - outer_contract(lines[:, :rank], lines, HIGHEST)
            return carry

        lax.fori_loop(first, last, panel, 0)

    for it in range(ITERS):
        order = (y_far, y_up, y_dn, my)

        def pair(n):
            for k in (ok, mk):
                g = order[n] * NK + k
                base = pl.multiple_of(g * shard, TILE)
                if it == 0:
                    residuals(g)
                part = jnp.dot(omega[...], res[:, pl.ds(base, shard)], preferred_element_type=F32)
                if k is ok:
                    psend[it, n] = part
                    out = copy(
                        psend.at[it, n], precv.at[it, n], pr_ss.at[it, n], pr_rs.at[it, n], *g_peer(my * NK + ok)
                    )
                    out.start()
                    sent.append(out)
                else:
                    pown[n] = part

        def both(n):
            copy(
                psend.at[it, n], precv.at[it, n], pr_ss.at[it, n], pr_rs.at[it, n], *g_peer(my * NK + ok)
            ).wait_recv()
            return pown[n] + precv[it, n]

        up, dn = g_peer(y_up * NK + mk), g_peer(y_dn * NK + mk)
        other = g_peer(my * NK + ok)
        top, bot = pl.ds(0, half), pl.ds(half, half)

        def hop(src, dst, n, peer):
            out = copy(src, dst, f_ss.at[it, n], f_rs.at[it, n], *peer)
            out.start()
            sent.append(out)
            return out

        pair(0)
        pair(1)
        qbuf[it, 0] = both(0).astype(BF16)
        far_up = hop(qbuf.at[it, 0, top], fbuf.at[it, 0], 0, up)
        far_dn = hop(qbuf.at[it, 0, bot], fbuf.at[it, 1], 1, dn)
        q = both(1)
        qbuf[it, 1, bot] = q[half:].astype(BF16)
        late[0] = q[:half]
        free_up = hop(qbuf.at[it, 1, bot], rbuf.at[it, 0, bot], 2, up)
        pair(2)
        q = both(2)
        qbuf[it, 2, top] = q[:half].astype(BF16)
        late[1] = q[half:]
        free_dn = hop(qbuf.at[it, 2, top], rbuf.at[it, 1, top], 3, dn)
        pair(3)
        far_up.wait_recv()
        qbuf[it, 1, top] = (late[0] + fbuf[it, 0].astype(F32)).astype(BF16)
        near_up = hop(qbuf.at[it, 1, top], rbuf.at[it, 0, top], 4, up)
        far_dn.wait_recv()
        qbuf[it, 2, bot] = (late[1] + fbuf[it, 1].astype(F32)).astype(BF16)
        near_dn = hop(qbuf.at[it, 2, bot], rbuf.at[it, 1, bot], 5, dn)
        own = both(3)
        for q in (free_up, free_dn, near_up, near_dn):
            q.wait_recv()
        sfull[it, me_g] = (own + rbuf[it, 0].astype(F32) + rbuf[it, 1].astype(F32)).astype(BF16)

        def block(g, first, n):
            return sfull.at[it, g, pl.ds(first * quarter, n * quarter)]

        def send(n, g, first, count, peer):
            out = copy(block(g, first, count), block(g, first, count), ag_ss.at[it, n], ag_rs.at[it, n], *peer)
            out.start()
            sent.append(out)

        def arrive(n, g, first, count):
            copy(
                block(g, first, count), block(g, first, count), ag_ss.at[it, n], ag_rs.at[it, n], *other
            ).wait_recv()

        mine = me_g
        up_k, dn_k, far_k = (y * NK + mk for y in (y_up, y_dn, y_far))
        up_o, dn_o, far_o = (y * NK + ok for y in (y_up, y_dn, y_far))
        mine_o = my * NK + ok

        def gather(first, g):
            base = pl.multiple_of(g * shard, TILE)
            t = inner_contract(res[:, pl.ds(base, shard)], sfull[it, g])
            tacc[...] = t if first else tacc[...] + t

        send(0, mine, 0, 1, up)
        send(3, mine, 2, 1, dn)
        send(1, mine, 1, 1, up)
        send(4, mine, 3, 1, dn)
        s = sfull[it, mine]
        gram = inner_contract(s, s)
        for i in range(ng):
            gsrc[it, i] = gram[i * gr : (i + 1) * gr, :]
        grow[it, me_g] = gsrc[it, me_g]
        got_gr = spread(ng, me_g, g_peer, lambda to: gsrc.at[it, to], grow.at[it], gr_ss.at[it], gr_rs.at[it])
        send(6, mine, 0, 4, other)
        send(2, mine, 2, 2, up)
        send(5, mine, 0, 2, dn)
        gather(True, mine)
        arrive(0, dn_k, 0, 1)
        send(7, dn_k, 0, 1, up)
        arrive(3, up_k, 2, 1)
        send(9, up_k, 2, 1, dn)
        arrive(1, dn_k, 1, 1)
        send(8, dn_k, 1, 1, up)
        arrive(4, up_k, 3, 1)
        send(10, up_k, 3, 1, dn)
        arrive(6, mine_o, 0, 4)
        gather(False, mine_o)
        wait_all(got_gr)
        gx[it, mx] = total([grow[it, i] for i in range(ng)], ng)
        got_gx = spread(nx, mx, x_peer, lambda to: gx.at[it, mx], gx.at[it], gx_ss.at[it], gx_rs.at[it])
        arrive(2, dn_k, 2, 2)
        send(11, dn_k, 0, 4, other)
        arrive(5, up_k, 0, 2)
        send(12, up_k, 0, 4, other)
        gather(False, dn_k)
        gather(False, up_k)
        arrive(11, dn_o, 0, 4)
        gather(False, dn_o)
        arrive(7, far_k, 0, 1)
        arrive(8, far_k, 1, 1)
        send(13, far_k, 0, 2, other)
        arrive(9, far_k, 2, 1)
        arrive(10, far_k, 3, 1)
        send(14, far_k, 2, 2, other)
        wait_all(got_gx)
        gz[it, mz] = total([gx[it, i] for i in range(nx)], nx)
        got_gz = spread(nz, mz, z_peer, lambda to: gz.at[it, mz], gz.at[it], gz_ss.at[it], gz_rs.at[it])
        arrive(12, up_o, 0, 4)
        gather(False, up_o)
        gather(False, far_k)
        arrive(13, far_o, 0, 2)
        arrive(14, far_o, 2, 2)
        gather(False, far_o)

        straight = it < ITERS - 1
        if straight:
            for i in range(nc):
                short_s[i] = tacc[pl.ds(i * piece, piece), :].astype(BF16)
            short_r[me_c] = short_s[me_c]
            got_tx = spread(nc, me_c, c_peer, lambda to: short_s.at[to], short_r, dr_ss, dr_rs)
        else:
            for i in range(nx):
                wide_s[i] = tacc[pl.ds(i * blk, blk), :]
            wide_r[mx] = wide_s[mx]
            got_tx = spread(nx, mx, x_peer, lambda to: wide_s.at[to], wide_r, tx_ss, tx_rs)
        wait_all(got_gz)
        gg[it, me_g] = total([gz[it, i] for i in range(nz)], nz)
        got_gg = spread(ng, me_g, g_peer, lambda to: gg.at[it, me_g], gg.at[it], gg_ss.at[it], gg_rs.at[it])
        wait_all(got_tx)
        if straight:
            tsum = total([short_r[i].astype(F32) for i in range(nc)], nc)
            short_all[me_c] = tsum.astype(BF16)
            got_all = spread(nc, me_c, c_peer, lambda to: short_all.at[me_c], short_all, da_ss, da_rs)
        else:
            tsum = total([wide_r[i] for i in range(nx)], nx)
            for i in range(nz):
                tzs[i] = tsum[i * zr : (i + 1) * zr, :]
            tzr[mz] = tzs[mz]
            got_tz = spread(nz, mz, z_peer, lambda to: tzs.at[to], tzr, tz_ss, tz_rs)
        if it == ITERS - 1:
            for i in range(ng):
                flat[i] = jnp.transpose(sfull[it, i])
            leave = pltpu.make_async_copy(flat, s_out, out_sem)
            leave.start()
        if not straight:
            wait_all(got_tz)
            wide_all[mx, mz] = total([tzr[i] for i in range(nz)], nz)
            got_taz = spread(nz, mz, z_peer, lambda to: wide_all.at[mx, mz], wide_all.at[mx], taz_ss, taz_rs)
        wait_all(got_gg)
        shift_gram(it)
        panels(0, rank // PANEL * 5 // 8)
        if not straight:
            wait_all(got_taz)
            got_all = spread(nx, mx, x_peer, lambda to: wide_all.at[mx], wide_all, tax_ss, tax_rs)
        panels(rank // PANEL * 5 // 8, rank // PANEL)
        white = linv[...] * math.sqrt(n_cells)
        front = jnp.transpose(white) if it == ITERS - 1 else white
        high = front.astype(BF16)
        low = (front - high.astype(F32)).astype(BF16)
        if it == ITERS - 1:
            w_out[:, pl.ds(0, rank)] = high
            w_out[:, pl.ds(rank, rank)] = low
        else:
            halves[pl.ds(0, rank), :] = high
            halves[pl.ds(rank, rank), :] = low
        wait_all(got_all)
        if straight:
            for i in range(nx):
                t = jnp.concatenate([short_all[i * nz + j] for j in range(nz)], axis=0)
                flip = inner_contract(halves[...], t)
                omega[:, pl.ds(i * blk, blk)] = ((flip[:rank] + flip[rank:]) * gene_scale).astype(BF16)
        else:
            for i in range(nx):
                t = jnp.concatenate([wide_all[i, j] for j in range(nz)], axis=0)
                load_out[pl.ds(i * blk, blk), :] = inner_contract(t, white, HIGHEST) * gene_scale

    leave.wait()
    for s in sent:
        s.wait_send()


def shard_of(rows, ng):
    return -(-rows // (ng * TILE)) * TILE


def finish(s_ref, white_ref, load_ref, basis_ref, out_ref):
    parts = jnp.dot(s_ref[...], white_ref[...], preferred_element_type=F32)
    rank = parts.shape[1] // 2
    basis_ref[...] = parts[:, :rank] + parts[:, rank:]
    out_ref[...] = load_ref[pl.ds(0, out_ref.shape[0]), :]


def shards(counts, sketch):
    rows, genes = counts.shape
    rank = sketch.shape[1]
    nc, ng = lax.axis_size("cells"), lax.axis_size("genes")
    nx = NX
    nz = nc // nx
    wide = -(-genes // TILE) * TILE
    shard = shard_of(rows, ng)
    blk, gr = wide // nx, rank // ng
    zr = blk // nz
    dims = (nx, nz, ng, rows, genes, wide, rank, nc * rows, ng * genes)
    V = pltpu.VMEM
    D = pltpu.SemaphoreType.DMA

    def pairs(*shape):
        return [D(shape), D(shape)]

    s_all, white, load = pl.pallas_call(
        functools.partial(kernel, dims),
        out_shape=(
            jax.ShapeDtypeStruct((ng, shard, rank), BF16),
            jax.ShapeDtypeStruct((rank, 2 * rank), BF16),
            jax.ShapeDtypeStruct((wide, rank), F32),
        ),
        in_specs=[pl.BlockSpec(memory_space=pl.ANY), pl.BlockSpec(memory_space=pltpu.VMEM)],
        out_specs=(
            pl.BlockSpec(memory_space=pl.ANY),
            pl.BlockSpec(memory_space=pltpu.VMEM),
            pl.BlockSpec(memory_space=pltpu.VMEM),
        ),
        scratch_shapes=[
            V((genes, rows), jnp.int32),
            V((wide, ng * shard), BF16),
            V((genes, TILE), jnp.int32),
            V((ng, 1, rows), F32),
            V((1, rows), F32),
            V((nc, 1, wide), F32),
            V((ng, 1, TILE), F32),
            V((wide, TILE), F32),
            V((rank, wide), BF16),
            V((ITERS, 4, rank, shard), F32),
            V((ITERS, 4, rank, shard), F32),
            V((4, rank, shard), F32),
            V((ITERS, 3, rank, shard), BF16),
            V((ITERS, 2, rank // 2, shard), BF16),
            V((ITERS, 2, rank, shard), BF16),
            V((2, rank // 2, shard), F32),
            V((ITERS, ng, rank, shard), BF16),
            V((ng, shard, rank), BF16),
            V((wide, rank), F32),
            V((ITERS, ng, gr, rank), F32),
            V((ITERS, ng, gr, rank), F32),
            V((nc, wide // nc, rank), BF16),
            V((nc, wide // nc, rank), BF16),
            V((nc, wide // nc, rank), BF16),
            V((nx, blk, rank), F32),
            V((nx, blk, rank), F32),
            V((nx, nz, zr, rank), F32),
            V((nz, zr, rank), F32),
            V((nz, zr, rank), F32),
            V((2 * rank, rank), BF16),
            V((ITERS, nx, gr, rank), F32),
            V((ITERS, nz, gr, rank), F32),
            V((ITERS, ng, gr, rank), F32),
            V((rank, 2 * rank), F32),
            V((rank, rank), F32),
            D((rows // (PER * TILE),)),
            D,
            *pairs(nc),
            *pairs(ng),
            *pairs(ng),
            *pairs(ITERS, 4),
            *pairs(ITERS, 6),
            *pairs(ITERS, 15),
            *pairs(nc),
            *pairs(nc),
            *pairs(nx),
            *pairs(nz),
            *pairs(nz),
            *pairs(nx),
            *pairs(ITERS, ng),
            *pairs(ITERS, nx),
            *pairs(ITERS, nz),
            *pairs(ITERS, ng),
        ],
        compiler_params=pltpu.CompilerParams(
            collective_id=0, has_side_effects=True, vmem_limit_bytes=60 * 2**20
        ),
        name="sweep",
    )(counts.T, sketch)
    step = rows // BLOCKS
    return pl.pallas_call(
        finish,
        grid=(BLOCKS,),
        out_shape=(
            jax.ShapeDtypeStruct((rows, rank), F32),
            jax.ShapeDtypeStruct((genes, rank), F32),
        ),
        in_specs=[
            pl.BlockSpec((step, rank), lambda i: (i, 0)),
            pl.BlockSpec((rank, 2 * rank), lambda i: (0, 0)),
            pl.BlockSpec((wide, rank), lambda i: (0, 0)),
        ],
        out_specs=(
            pl.BlockSpec((step, rank), lambda i: (i, 0)),
            pl.BlockSpec((genes, rank), lambda i: (0, 0)),
        ),
        name="finish",
    )(s_all.reshape(ng * shard, rank), white, load)


def solution(mesh):
    return jax.shard_map(
        shards,
        mesh=mesh,
        in_specs=(P("cells", "genes"), P("genes", None)),
        out_specs=(P("cells", None), P("genes", None)),
        check_vma=False,
    )
```

```python
import functools
import math

import jax
import jax.numpy as jnp
from jax import lax
from jax.experimental import pallas as pl
from jax.experimental.pallas import tpu as pltpu
from jax.sharding import PartitionSpec as P

ITERS = 2
NX = 4
NK = 2
TILE = 128
STEP = 32
PANEL = 8
PER = 2
BLOCKS = 2
HIGHEST = lax.Precision.HIGHEST
MESH = pl.DeviceIdType.MESH
F32 = jnp.float32
BF16 = jnp.bfloat16


def outer_contract(left, right, precision=None):
    return lax.dot_general(
        left, right, (((0,), (0,)), ((), ())), precision=precision, preferred_element_type=F32
    )


def inner_contract(left, right, precision=None):
    return lax.dot_general(
        left, right, (((1,), (1,)), ((), ())), precision=precision, preferred_element_type=F32
    )


def kernel(
    dims,
    counts_hbm,
    sketch_hbm,
    s_out,
    w_out,
    load_out,
    cnt,
    res,
    gpart,
    cellx,
    totc,
    genec,
    grp,
    fracs,
    omega,
    psend,
    precv,
    pown,
    qbuf,
    fbuf,
    rbuf,
    late,
    sfull,
    flat,
    tacc,
    gsrc,
    grow,
    short_s,
    short_r,
    short_all,
    wide_s,
    wide_r,
    wide_all,
    tzs,
    tzr,
    halves,
    gx,
    gz,
    gg,
    aug,
    linv,
    sketch,
    load_sem,
    take_sem,
    out_sem,
    bx_ss,
    bx_rs,
    ba_ss,
    ba_rs,
    bg_ss,
    bg_rs,
    pr_ss,
    pr_rs,
    f_ss,
    f_rs,
    ag_ss,
    ag_rs,
    dr_ss,
    dr_rs,
    da_ss,
    da_rs,
    tx_ss,
    tx_rs,
    tz_ss,
    tz_rs,
    taz_ss,
    taz_rs,
    tax_ss,
    tax_rs,
    gr_ss,
    gr_rs,
    gx_ss,
    gx_rs,
    gz_ss,
    gz_rs,
    gg_ss,
    gg_rs,
):
    nx, nz, ng, rows, genes, wide, rank, n_cells, n_genes = dims
    ny = ng // NK
    nc = nx * nz
    shard = shard_of(rows, ng)
    half, quarter = rank // 2, rank // 4
    blk = wide // nx
    zr = blk // nz
    gr = rank // ng
    me_c = lax.axis_index("cells")
    me_g = lax.axis_index("genes")
    mz, mx = me_c // nx, lax.rem(me_c, nx)
    my, mk = me_g // NK, lax.rem(me_g, NK)
    ok = 1 - mk
    y_up, y_dn, y_far = (lax.rem(my + d, ny) for d in (1, 3, 2))

    def copy(src, dst, ss, rs, c, g):
        return pltpu.make_async_remote_copy(
            src_ref=src, dst_ref=dst, send_sem=ss, recv_sem=rs, device_id=(c, g), device_id_type=MESH
        )

    def c_peer(i):
        return i, me_g

    def x_peer(i):
        return mz * nx + i, me_g

    def z_peer(i):
        return i * nx + mx, me_g

    def g_peer(i):
        return me_c, i

    sent = []

    def spread(n, me, peer, src_of, dst, ss, rs):
        arrivals = []
        for d in range(1, n):
            to, frm = lax.rem(me + d, n), lax.rem(me + n - d, n)
            out = copy(src_of(to), dst.at[me], ss.at[d], rs.at[d], *peer(to))
            out.start()
            sent.append(out)
            arrivals.append(copy(src_of(to), dst.at[frm], ss.at[d], rs.at[d], *peer(to)))
        return arrivals

    def wait_all(arrivals):
        for a in arrivals:
            a.wait_recv()

    def total(slots, n):
        acc = slots[0]
        for i in range(1, n):
            acc = acc + slots[i]
        return acc

    per = PER * TILE
    loads = rows // per

    def load(i):
        part = pl.ds(pl.multiple_of(i * per, TILE), per)
        return pltpu.make_async_copy(counts_hbm.at[:, part], cnt.at[:, part], load_sem.at[i])

    for i in range(loads):
        load(i).start()
    take = pltpu.make_async_copy(sketch_hbm, sketch, take_sem)
    take.start()

    barrier = pltpu.get_barrier_semaphore()
    for n, me, peer in ((nc, me_c, c_peer), (ng, me_g, g_peer)):
        for d in range(1, n):
            pl.semaphore_signal(barrier, inc=1, device_id=peer(lax.rem(me + d, n)), device_id_type=MESH)

    res[:, pl.ds(rows, ng * shard - rows)] = jnp.zeros((wide, ng * shard - rows), BF16)
    gpart[...] = jnp.zeros((genes, TILE), jnp.int32)
    even = genes - genes % 8

    def stats(i, carry):
        load(i).wait()
        tot = None
        for j in range(PER):
            at = pl.multiple_of(i * per + j * TILE, TILE)
            x = cnt[:, pl.ds(at, TILE)]
            tot = x if tot is None else tot + x
            down = jnp.sum(x[:even].reshape(even // 8, 8, TILE), axis=0)
            down = jnp.sum(down, axis=0, keepdims=True)
            if even < genes:
                down = down + jnp.sum(x[even:], axis=0, keepdims=True)
            cellx[me_g, :, pl.ds(at, TILE)] = down.astype(F32)
        gpart[...] = gpart[...] + tot
        return carry

    lax.fori_loop(0, loads, stats, 0)
    groups = wide // TILE
    for g in range(groups):
        n = min(TILE, genes - g * TILE)
        line = gpart[pl.ds(g * TILE, n), :].astype(F32)
        if n < TILE:
            line = jnp.concatenate([line, jnp.zeros((TILE - n, TILE), F32)], axis=0)
        genec[me_c, :, pl.ds(g * TILE, TILE)] = jnp.sum(jnp.transpose(line), axis=0, keepdims=True)

    pl.semaphore_wait(barrier, nc + ng - 2)
    got_c = spread(nc, me_c, c_peer, lambda to: genec.at[me_c], genec, bx_ss, bx_rs)
    got_a = spread(ng, me_g, g_peer, lambda to: cellx.at[me_g], cellx, ba_ss, ba_rs)
    take.wait()
    flip = jnp.transpose(sketch[...].astype(F32))
    omega[...] = jnp.concatenate([flip, jnp.zeros((rank, wide - genes), F32)], axis=1).astype(BF16)
    wait_all(got_a)
    totc[...] = total(cellx, ng)
    wait_all(got_c)
    gene_total = total(genec, nc)
    short = gene_total[:, :TILE]
    for g in range(1, groups):
        short = short + gene_total[:, g * TILE : (g + 1) * TILE]
    grp[me_g] = short
    got_g = spread(ng, me_g, g_peer, lambda to: grp.at[me_g], grp, bg_ss, bg_rs)
    fill = lax.broadcasted_iota(jnp.int32, (1, wide), 1) >= genes
    gene_total = jnp.where(fill, 1.0, gene_total)
    for g in range(groups):
        line = jnp.broadcast_to(gene_total[:, g * TILE : (g + 1) * TILE], (TILE, TILE))
        fracs[pl.ds(g * TILE, TILE), :] = jnp.transpose(line)
    wait_all(got_g)
    grand = jnp.sum(total(grp, ng), axis=1, keepdims=True)
    fracs[...] = fracs[...] / grand

    limit = math.sqrt(n_cells)

    def residuals(g):
        def some(t, carry):
            at = pl.ds(pl.multiple_of(t * TILE, TILE), TILE)
            cell = totc[:, at]
            for k in range(wide // STEP):
                n = min(STEP, genes - k * STEP)
                x = cnt[pl.ds(k * STEP, n), at].astype(F32)
                if n < STEP:
                    x = jnp.concatenate([x, jnp.zeros((STEP - n, TILE), F32)], axis=0)
                mu = cell * fracs[pl.ds(k * STEP, STEP), :]
                value = (x - mu) * lax.rsqrt(mu + 0.01 * mu * mu)
                value = jnp.clip(value, -limit, limit)
                if n < STEP:
                    row = lax.broadcasted_iota(jnp.int32, (STEP, TILE), 0)
                    value = jnp.where(row < n, value, 0.0)
                res[pl.ds(k * STEP, STEP), at] = value.astype(BF16)
            return carry

        first = g * (shard // TILE)
        lax.fori_loop(first, jnp.minimum(first + shard // TILE, rows // TILE), some, 0)

    gene_scale = math.sqrt(n_genes) / n_cells
    piece = wide // nc

    def shift_gram(it):
        eye = (
            lax.broadcasted_iota(jnp.int32, (rank, rank), 0)
            == lax.broadcasted_iota(jnp.int32, (rank, rank), 1)
        )
        gram = jnp.concatenate([gg[it, i] for i in range(ng)], axis=0)
        diagonal = jnp.sum(jnp.sum(jnp.where(eye, gram, 0.0), axis=1, keepdims=True), axis=0, keepdims=True)
        aug[:, pl.ds(0, rank)] = gram + jnp.where(eye, 1e-05 * diagonal / rank, 0.0)
        aug[:, pl.ds(rank, rank)] = jnp.where(eye, 1.0, 0.0)

    def panels(first, last):
        lane = lax.broadcasted_iota(jnp.int32, (PANEL, rank), 1)
        row = lax.broadcasted_iota(jnp.int32, (PANEL, 2 * rank), 0)

        def panel(p, carry):
            j = pl.multiple_of(p * PANEL, PANEL)
            lines = aug[pl.ds(j, PANEL), :]
            left = lines[:, :rank]
            heads = [
                jnp.sum(jnp.where(lane == j + i, left, 0.0), axis=1, keepdims=True) for i in range(PANEL)
            ]
            for i in range(PANEL):
                inv = lax.rsqrt(heads[i][i : i + 1, :])
                col = heads[i] * inv
                for m in range(i + 1, PANEL):
                    heads[m] = heads[m] - col * col[m : m + 1, :]
                this = lines[i : i + 1, :] * inv
                lines = jnp.where(row > i, lines - col * this, jnp.where(row == i, this, lines))
            linv[pl.ds(j, PANEL), :] = lines[:, rank:]
            aug[...] = aug[...] - outer_contract(lines[:, :rank], lines, HIGHEST)
            return carry

        lax.fori_loop(first, last, panel, 0)

    for it in range(ITERS):
        order = (y_far, y_up, y_dn, my)

        def part(n, k):
            g = order[n] * NK + k
            base = pl.multiple_of(g * shard, TILE)
            if it == 0:
                residuals(g)
            sums = jnp.dot(omega[...], res[:, pl.ds(base, shard)], preferred_element_type=F32)
            if k is ok:
                psend[it, n] = sums
                out = copy(
                    psend.at[it, n], precv.at[it, n], pr_ss.at[it, n], pr_rs.at[it, n], *g_peer(my * NK + ok)
                )
                out.start()
                sent.append(out)
            else:
                pown[n] = sums

        def both(n):
            copy(
                psend.at[it, n], precv.at[it, n], pr_ss.at[it, n], pr_rs.at[it, n], *g_peer(my * NK + ok)
            ).wait_recv()
            return pown[n] + precv[it, n]

        up, dn = g_peer(y_up * NK + mk), g_peer(y_dn * NK + mk)
        other = g_peer(my * NK + ok)
        top, bot = pl.ds(0, half), pl.ds(half, half)

        def hop(src, dst, n, peer):
            out = copy(src, dst, f_ss.at[it, n], f_rs.at[it, n], *peer)
            out.start()
            sent.append(out)
            return out

        part(0, ok)
        part(0, mk)
        part(1, ok)
        if it > 0:
            part(2, ok)
        qbuf[it, 0] = both(0).astype(BF16)
        far_up = hop(qbuf.at[it, 0, top], fbuf.at[it, 0], 0, up)
        far_dn = hop(qbuf.at[it, 0, bot], fbuf.at[it, 1], 1, dn)
        if it == 0:
            part(2, ok)
        part(1, mk)
        q = both(1)
        qbuf[it, 1, bot] = q[half:].astype(BF16)
        late[0] = q[:half]
        free_up = hop(qbuf.at[it, 1, bot], rbuf.at[it, 0, bot], 2, up)
        part(2, mk)
        q = both(2)
        qbuf[it, 2, top] = q[:half].astype(BF16)
        late[1] = q[half:]
        free_dn = hop(qbuf.at[it, 2, top], rbuf.at[it, 1, top], 3, dn)
        part(3, ok)
        part(3, mk)
        far_up.wait_recv()
        qbuf[it, 1, top] = (late[0] + fbuf[it, 0].astype(F32)).astype(BF16)
        near_up = hop(qbuf.at[it, 1, top], rbuf.at[it, 0, top], 4, up)
        far_dn.wait_recv()
        qbuf[it, 2, bot] = (late[1] + fbuf[it, 1].astype(F32)).astype(BF16)
        near_dn = hop(qbuf.at[it, 2, bot], rbuf.at[it, 1, bot], 5, dn)
        own = both(3)
        for q in (free_up, free_dn, near_up, near_dn):
            q.wait_recv()
        sfull[it, me_g] = (own + rbuf[it, 0].astype(F32) + rbuf[it, 1].astype(F32)).astype(BF16)

        def block(g, first, n):
            return sfull.at[it, g, pl.ds(first * quarter, n * quarter)]

        def send(n, g, first, count, peer):
            out = copy(block(g, first, count), block(g, first, count), ag_ss.at[it, n], ag_rs.at[it, n], *peer)
            out.start()
            sent.append(out)

        def arrive(n, g, first, count):
            copy(
                block(g, first, count), block(g, first, count), ag_ss.at[it, n], ag_rs.at[it, n], *other
            ).wait_recv()

        mine = me_g
        up_k, dn_k, far_k = (y * NK + mk for y in (y_up, y_dn, y_far))
        up_o, dn_o, far_o = (y * NK + ok for y in (y_up, y_dn, y_far))
        mine_o = my * NK + ok

        def gather(first, g):
            base = pl.multiple_of(g * shard, TILE)
            t = inner_contract(res[:, pl.ds(base, shard)], sfull[it, g])
            tacc[...] = t if first else tacc[...] + t

        send(0, mine, 0, 1, up)
        send(3, mine, 2, 1, dn)
        send(1, mine, 1, 1, up)
        send(4, mine, 3, 1, dn)
        s = sfull[it, mine]
        gram = inner_contract(s, s)
        for i in range(ng):
            gsrc[it, i] = gram[i * gr : (i + 1) * gr, :]
        grow[it, me_g] = gsrc[it, me_g]
        got_gr = spread(ng, me_g, g_peer, lambda to: gsrc.at[it, to], grow.at[it], gr_ss.at[it], gr_rs.at[it])
        send(6, mine, 0, 4, other)
        send(2, mine, 2, 2, up)
        send(5, mine, 0, 2, dn)
        gather(True, mine)
        arrive(0, dn_k, 0, 1)
        send(7, dn_k, 0, 1, up)
        arrive(3, up_k, 2, 1)
        send(9, up_k, 2, 1, dn)
        arrive(1, dn_k, 1, 1)
        send(8, dn_k, 1, 1, up)
        arrive(4, up_k, 3, 1)
        send(10, up_k, 3, 1, dn)
        arrive(6, mine_o, 0, 4)
        gather(False, mine_o)
        wait_all(got_gr)
        gx[it, mx] = total([grow[it, i] for i in range(ng)], ng)
        got_gx = spread(nx, mx, x_peer, lambda to: gx.at[it, mx], gx.at[it], gx_ss.at[it], gx_rs.at[it])
        arrive(2, dn_k, 2, 2)
        send(11, dn_k, 0, 4, other)
        arrive(5, up_k, 0, 2)
        send(12, up_k, 0, 4, other)
        gather(False, dn_k)
        gather(False, up_k)
        arrive(11, dn_o, 0, 4)
        gather(False, dn_o)
        arrive(7, far_k, 0, 1)
        arrive(8, far_k, 1, 1)
        send(13, far_k, 0, 2, other)
        arrive(9, far_k, 2, 1)
        arrive(10, far_k, 3, 1)
        send(14, far_k, 2, 2, other)
        wait_all(got_gx)
        gz[it, mz] = total([gx[it, i] for i in range(nx)], nx)
        got_gz = spread(nz, mz, z_peer, lambda to: gz.at[it, mz], gz.at[it], gz_ss.at[it], gz_rs.at[it])
        arrive(12, up_o, 0, 4)
        gather(False, up_o)
        gather(False, far_k)
        arrive(13, far_o, 0, 2)
        arrive(14, far_o, 2, 2)
        gather(False, far_o)

        straight = it < ITERS - 1
        if straight:
            for i in range(nc):
                short_s[i] = tacc[pl.ds(i * piece, piece), :].astype(BF16)
            short_r[me_c] = short_s[me_c]
            got_tx = spread(nc, me_c, c_peer, lambda to: short_s.at[to], short_r, dr_ss, dr_rs)
        else:
            for i in range(nx):
                wide_s[i] = tacc[pl.ds(i * blk, blk), :]
            wide_r[mx] = wide_s[mx]
            got_tx = spread(nx, mx, x_peer, lambda to: wide_s.at[to], wide_r, tx_ss, tx_rs)
        wait_all(got_gz)
        gg[it, me_g] = total([gz[it, i] for i in range(nz)], nz)
        got_gg = spread(ng, me_g, g_peer, lambda to: gg.at[it, me_g], gg.at[it], gg_ss.at[it], gg_rs.at[it])
        wait_all(got_tx)
        if straight:
            tsum = total([short_r[i].astype(F32) for i in range(nc)], nc)
            short_all[me_c] = tsum.astype(BF16)
            got_all = spread(nc, me_c, c_peer, lambda to: short_all.at[me_c], short_all, da_ss, da_rs)
        else:
            tsum = total([wide_r[i] for i in range(nx)], nx)
            for i in range(nz):
                tzs[i] = tsum[i * zr : (i + 1) * zr, :]
            tzr[mz] = tzs[mz]
            got_tz = spread(nz, mz, z_peer, lambda to: tzs.at[to], tzr, tz_ss, tz_rs)
        if it == ITERS - 1:
            for i in range(ng):
                flat[i] = jnp.transpose(sfull[it, i])
            leave = pltpu.make_async_copy(flat, s_out, out_sem)
            leave.start()
        if not straight:
            wait_all(got_tz)
            wide_all[mx, mz] = total([tzr[i] for i in range(nz)], nz)
            got_taz = spread(nz, mz, z_peer, lambda to: wide_all.at[mx, mz], wide_all.at[mx], taz_ss, taz_rs)
        wait_all(got_gg)
        shift_gram(it)
        panels(0, rank // PANEL * 5 // 8)
        if not straight:
            wait_all(got_taz)
            got_all = spread(nx, mx, x_peer, lambda to: wide_all.at[mx], wide_all, tax_ss, tax_rs)
        panels(rank // PANEL * 5 // 8, rank // PANEL)
        white = linv[...] * math.sqrt(n_cells)
        front = jnp.transpose(white) if it == ITERS - 1 else white
        high = front.astype(BF16)
        low = (front - high.astype(F32)).astype(BF16)
        if it == ITERS - 1:
            w_out[:, pl.ds(0, rank)] = high
            w_out[:, pl.ds(rank, rank)] = low
        else:
            halves[pl.ds(0, rank), :] = high
            halves[pl.ds(rank, rank), :] = low
        wait_all(got_all)
        if straight:
            for i in range(nx):
                t = jnp.concatenate([short_all[i * nz + j] for j in range(nz)], axis=0)
                flip = inner_contract(halves[...], t)
                omega[:, pl.ds(i * blk, blk)] = ((flip[:rank] + flip[rank:]) * gene_scale).astype(BF16)
        else:
            for i in range(nx):
                t = jnp.concatenate([wide_all[i, j] for j in range(nz)], axis=0)
                load_out[pl.ds(i * blk, blk), :] = inner_contract(t, white, HIGHEST) * gene_scale

    leave.wait()
    for s in sent:
        s.wait_send()


def shard_of(rows, ng):
    return -(-rows // (ng * TILE)) * TILE


def finish(s_ref, white_ref, load_ref, basis_ref, out_ref):
    parts = jnp.dot(s_ref[...], white_ref[...], preferred_element_type=F32)
    rank = parts.shape[1] // 2
    basis_ref[...] = parts[:, :rank] + parts[:, rank:]
    out_ref[...] = load_ref[pl.ds(0, out_ref.shape[0]), :]


def shards(counts, sketch):
    rows, genes = counts.shape
    rank = sketch.shape[1]
    nc, ng = lax.axis_size("cells"), lax.axis_size("genes")
    nx = NX
    nz = nc // nx
    wide = -(-genes // TILE) * TILE
    shard = shard_of(rows, ng)
    blk, gr = wide // nx, rank // ng
    zr = blk // nz
    dims = (nx, nz, ng, rows, genes, wide, rank, nc * rows, ng * genes)
    V = pltpu.VMEM
    D = pltpu.SemaphoreType.DMA

    def pairs(*shape):
        return [D(shape), D(shape)]

    s_all, white, load = pl.pallas_call(
        functools.partial(kernel, dims),
        out_shape=(
            jax.ShapeDtypeStruct((ng, shard, rank), BF16),
            jax.ShapeDtypeStruct((rank, 2 * rank), BF16),
            jax.ShapeDtypeStruct((wide, rank), F32),
        ),
        in_specs=[pl.BlockSpec(memory_space=pl.ANY), pl.BlockSpec(memory_space=pl.ANY)],
        out_specs=(
            pl.BlockSpec(memory_space=pl.ANY),
            pl.BlockSpec(memory_space=pltpu.VMEM),
            pl.BlockSpec(memory_space=pltpu.VMEM),
        ),
        scratch_shapes=[
            V((genes, rows), jnp.int32),
            V((wide, ng * shard), BF16),
            V((genes, TILE), jnp.int32),
            V((ng, 1, rows), F32),
            V((1, rows), F32),
            V((nc, 1, wide), F32),
            V((ng, 1, TILE), F32),
            V((wide, TILE), F32),
            V((rank, wide), BF16),
            V((ITERS, 4, rank, shard), F32),
            V((ITERS, 4, rank, shard), F32),
            V((4, rank, shard), F32),
            V((ITERS, 3, rank, shard), BF16),
            V((ITERS, 2, rank // 2, shard), BF16),
            V((ITERS, 2, rank, shard), BF16),
            V((2, rank // 2, shard), F32),
            V((ITERS, ng, rank, shard), BF16),
            V((ng, shard, rank), BF16),
            V((wide, rank), F32),
            V((ITERS, ng, gr, rank), F32),
            V((ITERS, ng, gr, rank), F32),
            V((nc, wide // nc, rank), BF16),
            V((nc, wide // nc, rank), BF16),
            V((nc, wide // nc, rank), BF16),
            V((nx, blk, rank), F32),
            V((nx, blk, rank), F32),
            V((nx, nz, zr, rank), F32),
            V((nz, zr, rank), F32),
            V((nz, zr, rank), F32),
            V((2 * rank, rank), BF16),
            V((ITERS, nx, gr, rank), F32),
            V((ITERS, nz, gr, rank), F32),
            V((ITERS, ng, gr, rank), F32),
            V((rank, 2 * rank), F32),
            V((rank, rank), F32),
            V((genes, rank), BF16),
            D((rows // (PER * TILE),)),
            D,
            D,
            *pairs(nc),
            *pairs(ng),
            *pairs(ng),
            *pairs(ITERS, 4),
            *pairs(ITERS, 6),
            *pairs(ITERS, 15),
            *pairs(nc),
            *pairs(nc),
            *pairs(nx),
            *pairs(nz),
            *pairs(nz),
            *pairs(nx),
            *pairs(ITERS, ng),
            *pairs(ITERS, nx),
            *pairs(ITERS, nz),
            *pairs(ITERS, ng),
        ],
        compiler_params=pltpu.CompilerParams(
            collective_id=0, has_side_effects=True, vmem_limit_bytes=60 * 2**20
        ),
        name="sweep",
    )(counts.T, sketch)
    step = rows // BLOCKS
    return pl.pallas_call(
        finish,
        grid=(BLOCKS,),
        out_shape=(
            jax.ShapeDtypeStruct((rows, rank), F32),
            jax.ShapeDtypeStruct((genes, rank), F32),
        ),
        in_specs=[
            pl.BlockSpec((step, rank), lambda i: (i, 0)),
            pl.BlockSpec((rank, 2 * rank), lambda i: (0, 0)),
            pl.BlockSpec((wide, rank), lambda i: (0, 0)),
        ],
        out_specs=(
            pl.BlockSpec((step, rank), lambda i: (i, 0)),
            pl.BlockSpec((genes, rank), lambda i: (0, 0)),
        ),
        name="finish",
    )(s_all.reshape(ng * shard, rank), white, load)


def solution(mesh):
    return jax.shard_map(
        shards,
        mesh=mesh,
        in_specs=(P("cells", "genes"), P("genes", None)),
        out_specs=(P("cells", None), P("genes", None)),
        check_vma=False,
    )
```

```python
import functools
import math

import jax
import jax.numpy as jnp
from jax import lax
from jax.experimental import pallas as pl
from jax.experimental.pallas import tpu as pltpu
from jax.sharding import PartitionSpec as P

ITERS = 2
NX = 4
NK = 2
TILE = 128
STEP = 32
PANEL = 8
PER = 2
BLOCKS = 2
HIGHEST = lax.Precision.HIGHEST
MESH = pl.DeviceIdType.MESH
F32 = jnp.float32
BF16 = jnp.bfloat16


def outer_contract(left, right, precision=None):
    return lax.dot_general(
        left, right, (((0,), (0,)), ((), ())), precision=precision, preferred_element_type=F32
    )


def inner_contract(left, right, precision=None):
    return lax.dot_general(
        left, right, (((1,), (1,)), ((), ())), precision=precision, preferred_element_type=F32
    )


def kernel(
    dims,
    counts_hbm,
    sketch_hbm,
    s_out,
    w_out,
    load_out,
    cnt,
    res,
    gpart,
    cellx,
    totc,
    genec,
    grp,
    fracs,
    omega,
    psend,
    precv,
    pown,
    qbuf,
    fbuf,
    rbuf,
    late,
    sfull,
    flat,
    tacc,
    gsrc,
    grow,
    short_s,
    short_r,
    short_all,
    wide_s,
    wide_r,
    last,
    tzs,
    tzr,
    halves,
    gx,
    gz,
    gg,
    aug,
    linv,
    sketch,
    load_sem,
    take_sem,
    out_sem,
    bx_ss,
    bx_rs,
    ba_ss,
    ba_rs,
    bg_ss,
    bg_rs,
    pr_ss,
    pr_rs,
    f_ss,
    f_rs,
    ag_ss,
    ag_rs,
    dr_ss,
    dr_rs,
    da_ss,
    da_rs,
    tx_ss,
    tx_rs,
    tz_ss,
    tz_rs,
    la_ss,
    la_rs,
    gr_ss,
    gr_rs,
    gx_ss,
    gx_rs,
    gz_ss,
    gz_rs,
    gg_ss,
    gg_rs,
):
    nx, nz, ng, rows, genes, wide, rank, n_cells, n_genes = dims
    ny = ng // NK
    nc = nx * nz
    shard = shard_of(rows, ng)
    half, quarter = rank // 2, rank // 4
    blk = wide // nx
    zr = blk // nz
    gr = rank // ng
    me_c = lax.axis_index("cells")
    me_g = lax.axis_index("genes")
    mz, mx = me_c // nx, lax.rem(me_c, nx)
    my, mk = me_g // NK, lax.rem(me_g, NK)
    ok = 1 - mk
    y_up, y_dn, y_far = (lax.rem(my + d, ny) for d in (1, 3, 2))

    def copy(src, dst, ss, rs, c, g):
        return pltpu.make_async_remote_copy(
            src_ref=src, dst_ref=dst, send_sem=ss, recv_sem=rs, device_id=(c, g), device_id_type=MESH
        )

    def c_peer(i):
        return i, me_g

    def x_peer(i):
        return mz * nx + i, me_g

    def z_peer(i):
        return i * nx + mx, me_g

    def g_peer(i):
        return me_c, i

    sent = []

    def spread(n, me, peer, src_of, dst, ss, rs):
        arrivals = []
        for d in range(1, n):
            to, frm = lax.rem(me + d, n), lax.rem(me + n - d, n)
            out = copy(src_of(to), dst.at[me], ss.at[d], rs.at[d], *peer(to))
            out.start()
            sent.append(out)
            arrivals.append(copy(src_of(to), dst.at[frm], ss.at[d], rs.at[d], *peer(to)))
        return arrivals

    def wait_all(arrivals):
        for a in arrivals:
            a.wait_recv()

    def total(slots, n):
        acc = slots[0]
        for i in range(1, n):
            acc = acc + slots[i]
        return acc

    per = PER * TILE
    loads = rows // per

    def load(i):
        part = pl.ds(pl.multiple_of(i * per, TILE), per)
        return pltpu.make_async_copy(counts_hbm.at[:, part], cnt.at[:, part], load_sem.at[i])

    for i in range(loads):
        load(i).start()
    take = pltpu.make_async_copy(sketch_hbm, sketch, take_sem)
    take.start()

    barrier = pltpu.get_barrier_semaphore()
    for n, me, peer in ((nc, me_c, c_peer), (ng, me_g, g_peer)):
        for d in range(1, n):
            pl.semaphore_signal(barrier, inc=1, device_id=peer(lax.rem(me + d, n)), device_id_type=MESH)

    res[:, pl.ds(rows, ng * shard - rows)] = jnp.zeros((wide, ng * shard - rows), BF16)
    gpart[...] = jnp.zeros((genes, TILE), jnp.int32)
    even = genes - genes % 8

    def stats(i, carry):
        load(i).wait()
        tot = None
        for j in range(PER):
            at = pl.multiple_of(i * per + j * TILE, TILE)
            x = cnt[:, pl.ds(at, TILE)]
            tot = x if tot is None else tot + x
            down = jnp.sum(x[:even].reshape(even // 8, 8, TILE), axis=0)
            down = jnp.sum(down, axis=0, keepdims=True)
            if even < genes:
                down = down + jnp.sum(x[even:], axis=0, keepdims=True)
            cellx[me_g, :, pl.ds(at, TILE)] = down.astype(F32)
        gpart[...] = gpart[...] + tot
        return carry

    lax.fori_loop(0, loads, stats, 0)
    groups = wide // TILE
    for g in range(groups):
        n = min(TILE, genes - g * TILE)
        line = gpart[pl.ds(g * TILE, n), :].astype(F32)
        if n < TILE:
            line = jnp.concatenate([line, jnp.zeros((TILE - n, TILE), F32)], axis=0)
        genec[me_c, :, pl.ds(g * TILE, TILE)] = jnp.sum(jnp.transpose(line), axis=0, keepdims=True)

    pl.semaphore_wait(barrier, nc + ng - 2)
    got_c = spread(nc, me_c, c_peer, lambda to: genec.at[me_c], genec, bx_ss, bx_rs)
    got_a = spread(ng, me_g, g_peer, lambda to: cellx.at[me_g], cellx, ba_ss, ba_rs)
    take.wait()
    flip = jnp.transpose(sketch[...].astype(F32))
    omega[...] = jnp.concatenate([flip, jnp.zeros((rank, wide - genes), F32)], axis=1).astype(BF16)
    wait_all(got_a)
    totc[...] = total(cellx, ng)
    wait_all(got_c)
    gene_total = total(genec, nc)
    short = gene_total[:, :TILE]
    for g in range(1, groups):
        short = short + gene_total[:, g * TILE : (g + 1) * TILE]
    grp[me_g] = short
    got_g = spread(ng, me_g, g_peer, lambda to: grp.at[me_g], grp, bg_ss, bg_rs)
    fill = lax.broadcasted_iota(jnp.int32, (1, wide), 1) >= genes
    gene_total = jnp.where(fill, 1.0, gene_total)
    for g in range(groups):
        line = jnp.broadcast_to(gene_total[:, g * TILE : (g + 1) * TILE], (TILE, TILE))
        fracs[pl.ds(g * TILE, TILE), :] = jnp.transpose(line)
    wait_all(got_g)
    grand = jnp.sum(total(grp, ng), axis=1, keepdims=True)
    fracs[...] = fracs[...] / grand

    limit = math.sqrt(n_cells)

    def residuals(g):
        def some(t, carry):
            at = pl.ds(pl.multiple_of(t * TILE, TILE), TILE)
            cell = totc[:, at]
            for k in range(wide // STEP):
                n = min(STEP, genes - k * STEP)
                x = cnt[pl.ds(k * STEP, n), at].astype(F32)
                if n < STEP:
                    x = jnp.concatenate([x, jnp.zeros((STEP - n, TILE), F32)], axis=0)
                mu = cell * fracs[pl.ds(k * STEP, STEP), :]
                value = (x - mu) * lax.rsqrt(mu + 0.01 * mu * mu)
                value = jnp.clip(value, -limit, limit)
                if n < STEP:
                    row = lax.broadcasted_iota(jnp.int32, (STEP, TILE), 0)
                    value = jnp.where(row < n, value, 0.0)
                res[pl.ds(k * STEP, STEP), at] = value.astype(BF16)
            return carry

        first = g * (shard // TILE)
        lax.fori_loop(first, jnp.minimum(first + shard // TILE, rows // TILE), some, 0)

    gene_scale = math.sqrt(n_genes) / n_cells
    piece = wide // nc

    def shift_gram(it):
        eye = (
            lax.broadcasted_iota(jnp.int32, (rank, rank), 0)
            == lax.broadcasted_iota(jnp.int32, (rank, rank), 1)
        )
        gram = jnp.concatenate([gg[it, i] for i in range(ng)], axis=0)
        diagonal = jnp.sum(jnp.sum(jnp.where(eye, gram, 0.0), axis=1, keepdims=True), axis=0, keepdims=True)
        aug[:, pl.ds(0, rank)] = gram + jnp.where(eye, 1e-05 * diagonal / rank, 0.0)
        aug[:, pl.ds(rank, rank)] = jnp.where(eye, 1.0, 0.0)

    def panels(first, last):
        lane = lax.broadcasted_iota(jnp.int32, (PANEL, rank), 1)
        row = lax.broadcasted_iota(jnp.int32, (PANEL, 2 * rank), 0)

        def panel(p, carry):
            j = pl.multiple_of(p * PANEL, PANEL)
            lines = aug[pl.ds(j, PANEL), :]
            left = lines[:, :rank]
            heads = [
                jnp.sum(jnp.where(lane == j + i, left, 0.0), axis=1, keepdims=True) for i in range(PANEL)
            ]
            for i in range(PANEL):
                inv = lax.rsqrt(heads[i][i : i + 1, :])
                col = heads[i] * inv
                for m in range(i + 1, PANEL):
                    heads[m] = heads[m] - col * col[m : m + 1, :]
                this = lines[i : i + 1, :] * inv
                lines = jnp.where(row > i, lines - col * this, jnp.where(row == i, this, lines))
            linv[pl.ds(j, PANEL), :] = lines[:, rank:]
            aug[...] = aug[...] - outer_contract(lines[:, :rank], lines, HIGHEST)
            return carry

        lax.fori_loop(first, last, panel, 0)

    for it in range(ITERS):
        order = (y_far, y_up, y_dn, my)

        def part(n, k):
            g = order[n] * NK + k
            base = pl.multiple_of(g * shard, TILE)
            if it == 0:
                residuals(g)
            sums = jnp.dot(omega[...], res[:, pl.ds(base, shard)], preferred_element_type=F32)
            if k is ok:
                psend[it, n] = sums
                out = copy(
                    psend.at[it, n], precv.at[it, n], pr_ss.at[it, n], pr_rs.at[it, n], *g_peer(my * NK + ok)
                )
                out.start()
                sent.append(out)
            else:
                pown[n] = sums

        def both(n):
            copy(
                psend.at[it, n], precv.at[it, n], pr_ss.at[it, n], pr_rs.at[it, n], *g_peer(my * NK + ok)
            ).wait_recv()
            return pown[n] + precv[it, n]

        up, dn = g_peer(y_up * NK + mk), g_peer(y_dn * NK + mk)
        other = g_peer(my * NK + ok)
        top, bot = pl.ds(0, half), pl.ds(half, half)

        def hop(src, dst, n, peer):
            out = copy(src, dst, f_ss.at[it, n], f_rs.at[it, n], *peer)
            out.start()
            sent.append(out)
            return out

        part(0, ok)
        part(0, mk)
        part(1, ok)
        if it > 0:
            part(2, ok)
        qbuf[it, 0] = both(0).astype(BF16)
        far_up = hop(qbuf.at[it, 0, top], fbuf.at[it, 0], 0, up)
        far_dn = hop(qbuf.at[it, 0, bot], fbuf.at[it, 1], 1, dn)
        if it == 0:
            part(2, ok)
        part(1, mk)
        q = both(1)
        qbuf[it, 1, bot] = q[half:].astype(BF16)
        late[0] = q[:half]
        free_up = hop(qbuf.at[it, 1, bot], rbuf.at[it, 0, bot], 2, up)
        part(2, mk)
        q = both(2)
        qbuf[it, 2, top] = q[:half].astype(BF16)
        late[1] = q[half:]
        free_dn = hop(qbuf.at[it, 2, top], rbuf.at[it, 1, top], 3, dn)
        part(3, ok)
        part(3, mk)
        far_up.wait_recv()
        qbuf[it, 1, top] = (late[0] + fbuf[it, 0].astype(F32)).astype(BF16)
        near_up = hop(qbuf.at[it, 1, top], rbuf.at[it, 0, top], 4, up)
        far_dn.wait_recv()
        qbuf[it, 2, bot] = (late[1] + fbuf[it, 1].astype(F32)).astype(BF16)
        near_dn = hop(qbuf.at[it, 2, bot], rbuf.at[it, 1, bot], 5, dn)
        own = both(3)
        for q in (free_up, free_dn, near_up, near_dn):
            q.wait_recv()
        sfull[it, me_g] = (own + rbuf[it, 0].astype(F32) + rbuf[it, 1].astype(F32)).astype(BF16)

        def block(g, first, n):
            return sfull.at[it, g, pl.ds(first * quarter, n * quarter)]

        def send(n, g, first, count, peer):
            out = copy(block(g, first, count), block(g, first, count), ag_ss.at[it, n], ag_rs.at[it, n], *peer)
            out.start()
            sent.append(out)

        def arrive(n, g, first, count):
            copy(
                block(g, first, count), block(g, first, count), ag_ss.at[it, n], ag_rs.at[it, n], *other
            ).wait_recv()

        mine = me_g
        up_k, dn_k, far_k = (y * NK + mk for y in (y_up, y_dn, y_far))
        up_o, dn_o, far_o = (y * NK + ok for y in (y_up, y_dn, y_far))
        mine_o = my * NK + ok

        def gather(first, g):
            base = pl.multiple_of(g * shard, TILE)
            t = inner_contract(res[:, pl.ds(base, shard)], sfull[it, g])
            tacc[...] = t if first else tacc[...] + t

        send(0, mine, 0, 1, up)
        send(3, mine, 2, 1, dn)
        send(1, mine, 1, 1, up)
        send(4, mine, 3, 1, dn)
        s = sfull[it, mine]
        gram = inner_contract(s, s)
        for i in range(ng):
            gsrc[it, i] = gram[i * gr : (i + 1) * gr, :]
        grow[it, me_g] = gsrc[it, me_g]
        got_gr = spread(ng, me_g, g_peer, lambda to: gsrc.at[it, to], grow.at[it], gr_ss.at[it], gr_rs.at[it])
        send(6, mine, 0, 4, other)
        send(2, mine, 2, 2, up)
        send(5, mine, 0, 2, dn)
        gather(True, mine)
        arrive(0, dn_k, 0, 1)
        send(7, dn_k, 0, 1, up)
        arrive(3, up_k, 2, 1)
        send(9, up_k, 2, 1, dn)
        arrive(1, dn_k, 1, 1)
        send(8, dn_k, 1, 1, up)
        arrive(4, up_k, 3, 1)
        send(10, up_k, 3, 1, dn)
        arrive(6, mine_o, 0, 4)
        gather(False, mine_o)
        wait_all(got_gr)
        gx[it, mx] = total([grow[it, i] for i in range(ng)], ng)
        got_gx = spread(nx, mx, x_peer, lambda to: gx.at[it, mx], gx.at[it], gx_ss.at[it], gx_rs.at[it])
        arrive(2, dn_k, 2, 2)
        send(11, dn_k, 0, 4, other)
        arrive(5, up_k, 0, 2)
        send(12, up_k, 0, 4, other)
        gather(False, dn_k)
        gather(False, up_k)
        arrive(11, dn_o, 0, 4)
        gather(False, dn_o)
        arrive(7, far_k, 0, 1)
        arrive(8, far_k, 1, 1)
        send(13, far_k, 0, 2, other)
        arrive(9, far_k, 2, 1)
        arrive(10, far_k, 3, 1)
        send(14, far_k, 2, 2, other)
        wait_all(got_gx)
        gz[it, mz] = total([gx[it, i] for i in range(nx)], nx)
        got_gz = spread(nz, mz, z_peer, lambda to: gz.at[it, mz], gz.at[it], gz_ss.at[it], gz_rs.at[it])
        arrive(12, up_o, 0, 4)
        gather(False, up_o)
        gather(False, far_k)
        arrive(13, far_o, 0, 2)
        arrive(14, far_o, 2, 2)
        gather(False, far_o)

        straight = it < ITERS - 1
        if straight:
            for i in range(nc):
                short_s[i] = tacc[pl.ds(i * piece, piece), :].astype(BF16)
            short_r[me_c] = short_s[me_c]
            got_tx = spread(nc, me_c, c_peer, lambda to: short_s.at[to], short_r, dr_ss, dr_rs)
        else:
            for i in range(nx):
                wide_s[i] = tacc[pl.ds(i * blk, blk), :]
            wide_r[mx] = wide_s[mx]
            got_tx = spread(nx, mx, x_peer, lambda to: wide_s.at[to], wide_r, tx_ss, tx_rs)
        wait_all(got_gz)
        gg[it, me_g] = total([gz[it, i] for i in range(nz)], nz)
        got_gg = spread(ng, me_g, g_peer, lambda to: gg.at[it, me_g], gg.at[it], gg_ss.at[it], gg_rs.at[it])
        wait_all(got_tx)
        if straight:
            tsum = total([short_r[i].astype(F32) for i in range(nc)], nc)
            short_all[me_c] = tsum.astype(BF16)
            got_all = spread(nc, me_c, c_peer, lambda to: short_all.at[me_c], short_all, da_ss, da_rs)
        else:
            tsum = total([wide_r[i] for i in range(nx)], nx)
            for i in range(nz):
                tzs[i] = tsum[i * zr : (i + 1) * zr, :]
            tzr[mz] = tzs[mz]
            got_tz = spread(nz, mz, z_peer, lambda to: tzs.at[to], tzr, tz_ss, tz_rs)
        wait_all(got_gg)
        shift_gram(it)
        panels(0, rank // PANEL)
        white = linv[...] * math.sqrt(n_cells)
        if not straight:
            wait_all(got_tz)
            own = inner_contract(total([tzr[i] for i in range(nz)], nz), white, HIGHEST)
            last[me_c] = (own * gene_scale).astype(BF16)
            got_all = spread(nc, me_c, c_peer, lambda to: last.at[me_c], last, la_ss, la_rs)
            for i in range(ng):
                flat[i] = jnp.transpose(sfull[it, i])
            leave = pltpu.make_async_copy(flat, s_out, out_sem)
            leave.start()
        front = jnp.transpose(white) if it == ITERS - 1 else white
        high = front.astype(BF16)
        low = (front - high.astype(F32)).astype(BF16)
        if it == ITERS - 1:
            w_out[:, pl.ds(0, rank)] = high
            w_out[:, pl.ds(rank, rank)] = low
        else:
            halves[pl.ds(0, rank), :] = high
            halves[pl.ds(rank, rank), :] = low
        wait_all(got_all)
        if straight:
            for i in range(nx):
                t = jnp.concatenate([short_all[i * nz + j] for j in range(nz)], axis=0)
                flip = inner_contract(halves[...], t)
                omega[:, pl.ds(i * blk, blk)] = ((flip[:rank] + flip[rank:]) * gene_scale).astype(BF16)
        else:
            for i in range(nx):
                for j in range(nz):
                    load_out[pl.ds(i * blk + j * zr, zr), :] = last[j * nx + i].astype(F32)

    leave.wait()
    for s in sent:
        s.wait_send()


def shard_of(rows, ng):
    return -(-rows // (ng * TILE)) * TILE


def finish(s_ref, white_ref, load_ref, basis_ref, out_ref):
    parts = jnp.dot(s_ref[...], white_ref[...], preferred_element_type=F32)
    rank = parts.shape[1] // 2
    basis_ref[...] = parts[:, :rank] + parts[:, rank:]
    out_ref[...] = load_ref[pl.ds(0, out_ref.shape[0]), :]


def shards(counts, sketch):
    rows, genes = counts.shape
    rank = sketch.shape[1]
    nc, ng = lax.axis_size("cells"), lax.axis_size("genes")
    nx = NX
    nz = nc // nx
    wide = -(-genes // TILE) * TILE
    shard = shard_of(rows, ng)
    blk, gr = wide // nx, rank // ng
    zr = blk // nz
    dims = (nx, nz, ng, rows, genes, wide, rank, nc * rows, ng * genes)
    V = pltpu.VMEM
    D = pltpu.SemaphoreType.DMA

    def pairs(*shape):
        return [D(shape), D(shape)]

    s_all, white, load = pl.pallas_call(
        functools.partial(kernel, dims),
        out_shape=(
            jax.ShapeDtypeStruct((ng, shard, rank), BF16),
            jax.ShapeDtypeStruct((rank, 2 * rank), BF16),
            jax.ShapeDtypeStruct((wide, rank), F32),
        ),
        in_specs=[pl.BlockSpec(memory_space=pl.ANY), pl.BlockSpec(memory_space=pl.ANY)],
        out_specs=(
            pl.BlockSpec(memory_space=pl.ANY),
            pl.BlockSpec(memory_space=pltpu.VMEM),
            pl.BlockSpec(memory_space=pltpu.VMEM),
        ),
        scratch_shapes=[
            V((genes, rows), jnp.int32),
            V((wide, ng * shard), BF16),
            V((genes, TILE), jnp.int32),
            V((ng, 1, rows), F32),
            V((1, rows), F32),
            V((nc, 1, wide), F32),
            V((ng, 1, TILE), F32),
            V((wide, TILE), F32),
            V((rank, wide), BF16),
            V((ITERS, 4, rank, shard), F32),
            V((ITERS, 4, rank, shard), F32),
            V((4, rank, shard), F32),
            V((ITERS, 3, rank, shard), BF16),
            V((ITERS, 2, rank // 2, shard), BF16),
            V((ITERS, 2, rank, shard), BF16),
            V((2, rank // 2, shard), F32),
            V((ITERS, ng, rank, shard), BF16),
            V((ng, shard, rank), BF16),
            V((wide, rank), F32),
            V((ITERS, ng, gr, rank), F32),
            V((ITERS, ng, gr, rank), F32),
            V((nc, wide // nc, rank), BF16),
            V((nc, wide // nc, rank), BF16),
            V((nc, wide // nc, rank), BF16),
            V((nx, blk, rank), F32),
            V((nx, blk, rank), F32),
            V((nc, zr, rank), BF16),
            V((nz, zr, rank), F32),
            V((nz, zr, rank), F32),
            V((2 * rank, rank), BF16),
            V((ITERS, nx, gr, rank), F32),
            V((ITERS, nz, gr, rank), F32),
            V((ITERS, ng, gr, rank), F32),
            V((rank, 2 * rank), F32),
            V((rank, rank), F32),
            V((genes, rank), BF16),
            D((rows // (PER * TILE),)),
            D,
            D,
            *pairs(nc),
            *pairs(ng),
            *pairs(ng),
            *pairs(ITERS, 4),
            *pairs(ITERS, 6),
            *pairs(ITERS, 15),
            *pairs(nc),
            *pairs(nc),
            *pairs(nx),
            *pairs(nz),
            *pairs(nc),
            *pairs(ITERS, ng),
            *pairs(ITERS, nx),
            *pairs(ITERS, nz),
            *pairs(ITERS, ng),
        ],
        compiler_params=pltpu.CompilerParams(
            collective_id=0, has_side_effects=True, vmem_limit_bytes=60 * 2**20
        ),
        name="sweep",
    )(counts.T, sketch)
    step = rows // BLOCKS
    return pl.pallas_call(
        finish,
        grid=(BLOCKS,),
        out_shape=(
            jax.ShapeDtypeStruct((rows, rank), F32),
            jax.ShapeDtypeStruct((genes, rank), F32),
        ),
        in_specs=[
            pl.BlockSpec((step, rank), lambda i: (i, 0)),
            pl.BlockSpec((rank, 2 * rank), lambda i: (0, 0)),
            pl.BlockSpec((wide, rank), lambda i: (0, 0)),
        ],
        out_specs=(
            pl.BlockSpec((step, rank), lambda i: (i, 0)),
            pl.BlockSpec((genes, rank), lambda i: (0, 0)),
        ),
        name="finish",
    )(s_all.reshape(ng * shard, rank), white, load)


def solution(mesh):
    return jax.shard_map(
        shards,
        mesh=mesh,
        in_specs=(P("cells", "genes"), P("genes", None)),
        out_specs=(P("cells", None), P("genes", None)),
        check_vma=False,
    )
```
